256 devices in a mesh: grp: 16 (over y_lo, z), mem: 16 (over y_hi, x, core).
Axes of the slice: x: 4, y: 4 (y_hi: 2, y_lo: 2; y = y_hi * 2 + y_lo), z: 8, core: 2. Of those that a mesh axis runs over, the one named last changes fastest.
Arguments:
- client_input: bfloat16 [16, 16, 128, 896], P('grp', 'mem'), may hold values from -6 to 6
- client_gain: float32 [16, 896], P('mem'), may hold values from 0.5 to 1.5
- w_query: bfloat16 [16, 896, 896], P('mem'), may hold values from -1.5 to 1.5
- w_keyval: bfloat16 [16, 896, 256], P('mem'), may hold values from -0.5 to 0.5
- w_out: bfloat16 [16, 896, 896], P('mem'), may hold values from -0.1875 to 0.1875
- server_gain: float32 [16, 896], P('grp'), may hold values from 0.5 to 1.5
- w_gate: bfloat16 [16, 896, 4864], P('grp', None, 'mem'), may hold values from -0.1875 to 0.1875
- w_up: bfloat16 [16, 896, 4864], P('grp', None, 'mem'), may hold values from -0.1875 to 0.1875
- w_down: bfloat16 [16, 4864, 896], P('grp', 'mem'), may hold values from -0.078125 to 0.078125
- out_grad: bfloat16 [16, 16, 128, 896], P('grp', 'mem'), may hold values from -6 to 6
- valid: int32 [16, 16], P('grp', 'mem'), may hold values from 64 to 128
Outputs:
- server_out: bfloat16 [16, 16, 128, 896], P('grp', 'mem')
- grad_query: bfloat16 [16, 896, 896], P('mem')
- grad_keyval: bfloat16 [16, 896, 256], P('mem')
- grad_out: bfloat16 [16, 896, 896], P('mem')
- grad_gate: bfloat16 [16, 896, 4864], P('grp', None, 'mem')
- grad_up: bfloat16 [16, 896, 4864], P('grp', None, 'mem')
- grad_down: bfloat16 [16, 4864, 896], P('grp', 'mem')
The draws below stay inside these ranges and needn't reach their ends.
All inputs are finite; a program needn't handle non-finite values.
Results may differ from the reference program's by a relative error of at most 0.03.
Values may be sent and summed in bfloat16 or wider, within the bound.
A program may use at most 128 MiB of HBM per device.

```python
import jax
import jax.numpy as jnp
from jax import lax

D = 896
FF = 4864
KV_HEADS = 2
HEAD_DIM = 64
TOK = 128
GROUPS = 16
MEMBERS = 16


def query_tables(key):
    first, second = jax.random.split(jax.random.fold_in(key, 11))
    scale = D ** (-0.5)
    keyval = jax.random.normal(first, (MEMBERS, D, 2 * KV_HEADS * HEAD_DIM), jnp.float32) * scale
    query = jax.random.normal(second, (MEMBERS, D, D), jnp.float32) * scale
    return (jnp.clip(query, -1.5, 1.5), jnp.clip(keyval, -0.5, 0.5))


def draw_w_query(key, part):
    return query_tables(key)[0].astype(jnp.bfloat16)


def draw_w_keyval(key, part):
    return query_tables(key)[1].astype(jnp.bfloat16)


def touch_ends(drawn, stream_key, least, high):
    dims = drawn.shape
    index_at = [jax.random.randint(jax.random.fold_in(stream_key, axis), (), 0, dims[axis]) for axis in range(len(dims))]
    drawn = drawn.at[tuple(index_at)].set(least)
    longest = dims.index(max(dims))
    index_at[longest] = (index_at[longest] + 1) % dims[longest]
    return drawn.at[tuple(index_at)].set(high)


def shard_levels(key, extent, pieces, smallest, largest):
    gain, own = 1.0, jax.random.fold_in(key, 6)
    for axis_at, shards_of in pieces:
        steps = jnp.exp(jax.random.uniform(jax.random.fold_in(own, axis_at), (shards_of,), jnp.float32, smallest / len(pieces), largest / len(pieces)))
        gain = gain * jnp.repeat(steps, extent[axis_at] // shards_of).reshape([-1 if axis == axis_at else 1 for axis in range(len(extent))])
    return gain


def scatter_about(own_key, dims, scale, limit, pieces=(), held_as=jnp.bfloat16):
    values = scale * jax.random.normal(own_key, dims, jnp.float32)
    if pieces:
        values = values * shard_levels(own_key, dims, pieces, -0.22, 0.18)
    return jnp.clip(values, -limit, limit).astype(held_as)


def setup_inputs(seed: int = 0) -> dict:
    keys = jax.random.split(jax.random.key(seed), 12)
    return {
        "client_input": scatter_about(keys[0], (GROUPS, MEMBERS, TOK, D), 1.0, 6.0, ((0, 16), (1, 16))),
        "client_gain": jnp.clip(1.0 + 0.1 * jax.random.normal(keys[1], (MEMBERS, D), jnp.float32), 0.5, 1.5),
        "w_query": draw_w_query(jax.random.fold_in(keys[11], 71), 0),
        "w_keyval": draw_w_keyval(jax.random.fold_in(keys[11], 71), 0),
        "w_out": scatter_about(keys[4], (MEMBERS, D, D), D ** -0.5, 0.1875, ((0, 16),)),
        "server_gain": jnp.clip(1.0 + 0.1 * jax.random.normal(keys[5], (GROUPS, D), jnp.float32), 0.5, 1.5),
        "w_gate": scatter_about(keys[6], (GROUPS, D, FF), D ** -0.5, 0.1875, ((0, 16), (2, 16))),
        "w_up": scatter_about(keys[7], (GROUPS, D, FF), D ** -0.5, 0.1875, ((0, 16), (2, 16))),
        "w_down": scatter_about(keys[8], (GROUPS, FF, D), FF ** -0.5, 0.078125, ((0, 16), (1, 16))),
        "out_grad": scatter_about(keys[9], (GROUPS, MEMBERS, TOK, D), 1.0, 6.0, ((0, 16), (1, 16))),
        "valid": touch_ends(jax.random.randint(keys[10], (GROUPS, MEMBERS), TOK // 2, TOK + 1), jax.random.fold_in(keys[10], 1), TOK // 2, TOK).astype(jnp.int32),
    }


EPS = 1e-06

def client_forward(tokens_in, gain_vec, query_w, keyval_w, output_w):
    x_float = tokens_in.astype(jnp.float32)
    inv_rms = lax.rsqrt(lax.optimization_barrier(jnp.mean(x_float * x_float, axis=-1, keepdims=True)) + EPS)
    normed = (x_float * inv_rms * gain_vec).astype(jnp.bfloat16)
    queries = jnp.dot(normed, query_w, preferred_element_type=jnp.float32).astype(jnp.bfloat16)
    key_vals = jnp.dot(normed, keyval_w, preferred_element_type=jnp.float32).astype(jnp.bfloat16)
    length = tokens_in.shape[0]
    half_cols = KV_HEADS * HEAD_DIM
    q_heads = queries.reshape(length, KV_HEADS, -1, HEAD_DIM)
    k_heads = key_vals[:, :half_cols].reshape(length, KV_HEADS, HEAD_DIM)
    v_heads = key_vals[:, half_cols:].reshape(length, KV_HEADS, HEAD_DIM)
    scores = jnp.einsum('tgqd,sgd->gqts', q_heads.astype(jnp.float32), k_heads.astype(jnp.float32)) * HEAD_DIM ** (-0.5)
    causal = jnp.arange(length)[:, None] >= jnp.arange(length)[None, :]
    scores = jnp.where(causal, scores, -1e+30)
    highest = lax.optimization_barrier(jnp.max(scores, axis=-1, keepdims=True))
    expo = jnp.exp(scores - highest)
    probs = (expo / lax.optimization_barrier(jnp.sum(expo, axis=-1, keepdims=True))).astype(jnp.bfloat16)
    attended = jnp.einsum('gqts,sgd->tgqd', probs.astype(jnp.float32), v_heads.astype(jnp.float32))
    attended = attended.astype(jnp.bfloat16).reshape(length, -1)
    mixed = jnp.dot(attended, output_w, preferred_element_type=jnp.float32)
    return (x_float + mixed).astype(jnp.bfloat16)

def client_gradients(tokens_in, gain_vec, query_w, keyval_w, output_w, upstream):

    def inner(query_in, keyval_in, output_in):
        return client_forward(tokens_in, gain_vec, query_in, keyval_in, output_in)
    _, pull = jax.vjp(inner, query_w, keyval_w, output_w)
    return pull(upstream)

def norm_back(h_float, inv_rms, gain_vec, upstream):
    scaled = upstream * gain_vec
    return inv_rms * scaled - h_float * inv_rms ** 3 * lax.optimization_barrier(jnp.mean(scaled * h_float, axis=-1, keepdims=True))

def reference(client_input, client_gain, w_query, w_keyval, w_out, server_gain, w_gate, w_up, w_down, out_grad, valid):
    groups = client_input.shape[0]
    members = client_input.shape[1]
    length = client_input.shape[2]
    width = client_input.shape[3]
    positions = jnp.arange(length).astype(jnp.int32)

    def group_step(totals, group_in):
        x_group, s_gain, gate_w, up_w, down_w, cot_group, valid_group = group_in
        cuts = jax.vmap(client_forward)(x_group, client_gain, w_query, w_keyval, w_out)
        rows_cut = cuts.reshape(-1, width)
        h_float = rows_cut.astype(jnp.float32)
        inv_rms = lax.rsqrt(lax.optimization_barrier(jnp.mean(h_float * h_float, axis=-1, keepdims=True)) + EPS)
        normed = (h_float * inv_rms * s_gain).astype(jnp.bfloat16)
        gate_act = jnp.dot(normed, gate_w, preferred_element_type=jnp.float32)
        up_act = jnp.dot(normed, up_w, preferred_element_type=jnp.float32)
        sigma = jax.nn.sigmoid(gate_act)
        hidden = (gate_act * sigma * up_act).astype(jnp.bfloat16)
        server_rows = (h_float + jnp.dot(hidden, down_w, preferred_element_type=jnp.float32)).astype(jnp.bfloat16)
        live = positions[None, :] < valid_group[:, None]
        cot_rows = jnp.where(live[:, :, None], cot_group, jnp.zeros_like(cot_group)).reshape(-1, width)
        d_hidden = jnp.dot(cot_rows, down_w.T, preferred_element_type=jnp.float32)
        d_gate = (d_hidden * up_act * sigma * (1.0 + gate_act * (1.0 - sigma))).astype(jnp.bfloat16)
        d_up = (d_hidden * gate_act * sigma).astype(jnp.bfloat16)
        grad_down = jnp.dot(hidden.T, cot_rows, preferred_element_type=jnp.float32).astype(jnp.bfloat16)
        grad_gate = jnp.dot(normed.T, d_gate, preferred_element_type=jnp.float32).astype(jnp.bfloat16)
        grad_up = jnp.dot(normed.T, d_up, preferred_element_type=jnp.float32).astype(jnp.bfloat16)
        d_normed = jnp.dot(d_gate, gate_w.T, preferred_element_type=jnp.float32) + jnp.dot(d_up, up_w.T, preferred_element_type=jnp.float32)
        d_cut = cot_rows.astype(jnp.float32) + norm_back(h_float, inv_rms, s_gain, d_normed)
        cut_grad = (lax.optimization_barrier(jnp.sum(d_cut.reshape(members, length, width), axis=0)) / members).astype(jnp.bfloat16)
        grads = jax.vmap(client_gradients, in_axes=(0, 0, 0, 0, 0, None))(x_group, client_gain, w_query, w_keyval, w_out, cut_grad)
        new_totals = tuple((total + lax.optimization_barrier(piece).astype(jnp.float32) for total, piece in zip(totals, grads)))
        return (new_totals, (server_rows.reshape(members, length, width), grad_gate, grad_up, grad_down))
    start = (jnp.zeros(w_query.shape, jnp.float32), jnp.zeros(w_keyval.shape, jnp.float32), jnp.zeros(w_out.shape, jnp.float32))
    totals, stacked = lax.scan(group_step, start, (client_input, server_gain, w_gate, w_up, w_down, out_grad, valid))
    server_out, grad_gate, grad_up, grad_down = stacked
    grad_query = (totals[0] / groups).astype(jnp.bfloat16)
    grad_keyval = (totals[1] / groups).astype(jnp.bfloat16)
    grad_out = (totals[2] / groups).astype(jnp.bfloat16)
    return (server_out, grad_query, grad_keyval, grad_out, grad_gate, grad_up, grad_down)
```

```python
import functools

import jax
import jax.numpy as jnp
from jax import lax
from jax.experimental import pallas as pl
from jax.experimental.pallas import tpu as pltpu
from jax.sharding import PartitionSpec as P

EPS = 1e-06
HEAD_DIM = 64
TOK = 128
D = 896
PAIRS = 7
BF = jnp.bfloat16
F32 = jnp.float32
MESH = pl.DeviceIdType.MESH
NN = (((1,), (0,)), ((), ()))
NT = (((1,), (1,)), ((), ()))
TN = (((0,), (0,)), ((), ()))
HALF = TOK // 2


def mm(a, b, dims=NN):
    return lax.dot_general(a, b, dims, preferred_element_type=F32)


def places():
    g, m = lax.axis_index("grp"), lax.axis_index("mem")
    l, z = g // 8, g % 8
    yh, x, c = m // 8, (m // 2) % 4, m % 2
    at = lambda y_, x_, c_: {"mem": y_ * 8 + x_ * 2 + c_}
    return dict(
        m=m,
        c=c,
        xp=at(yh, (x + 1) % 4, c),
        xm=at(yh, (x + 3) % 4, c),
        x2=at(yh, (x + 2) % 4, c),
        yp=at(1 - yh, x, c),
        yxp=at(1 - yh, (x + 1) % 4, c),
        yxm=at(1 - yh, (x + 3) % 4, c),
        yx2=at(1 - yh, (x + 2) % 4, c),
        co=at(yh, x, 1 - c),
        zp={"grp": l * 8 + (z + 1) % 8},
        zm={"grp": l * 8 + (z + 7) % 8},
        lp={"grp": (1 - l) * 8 + z},
    )


def remote(src, dst, send, recv, k, device):
    return pltpu.make_async_remote_copy(
        src_ref=src, dst_ref=dst, send_sem=send.at[k], recv_sem=recv.at[k], device_id=device, device_id_type=MESH
    )


def entry_barrier(devices):
    barrier = pltpu.get_barrier_semaphore()
    for device in devices:
        pl.semaphore_signal(barrier, inc=1, device_id=device, device_id_type=MESH)
    pl.semaphore_wait(barrier, len(devices))


def ring_slot(step, stream, way):
    return 2 + 4 * (step - 1) + 2 * stream + way if step < 4 else 14 + stream


def stacked_heads(both):
    wide = both.astype(F32)
    turned = pltpu.roll(wide, HEAD_DIM, 1)
    low = lax.broadcasted_iota(jnp.int32, wide.shape, 1) < HEAD_DIM
    zero = jnp.zeros_like(wide)
    first0, second0 = jnp.where(low, wide, zero), jnp.where(low, zero, turned)
    first1, second1 = jnp.where(low, turned, zero), jnp.where(low, zero, wide)
    pair = lambda a, b: jnp.concatenate([a, b], axis=0).astype(BF)
    return pair(first0, second0), pair(first0, second1), pair(first1, second1)


def of_pair(p, three):
    return three[0] if p < 3 else three[1] if p == 3 else three[2]


def client_forward(i, x, gain, wq_ref, wkv_ref, nt_ref, at_ref, q_ref, kv_ref, pt_ref, att_ref):
    xf = x.astype(F32)
    inv = lax.rsqrt(jnp.mean(xf * xf, axis=-1, keepdims=True) + EPS)
    normed_f = (xf * inv * gain).astype(BF)
    columns = pl.ds(pl.multiple_of(i * TOK, TOK), TOK)
    nt_ref[:, columns] = normed_f.T
    q_ref[i] = mm(normed_f, wq_ref[...]).astype(BF)
    kv = mm(normed_f, wkv_ref[...]).astype(BF)
    kv_ref[i] = kv
    keys, vals = stacked_heads(kv[:, :TOK]), stacked_heads(kv[:, TOK:])
    s_at = lax.broadcasted_iota(jnp.int32, (TOK, TOK), 0)
    t_at = lax.broadcasted_iota(jnp.int32, (TOK, TOK), 1)
    seen = s_at <= t_at
    for p in range(PAIRS):
        cols = slice(p * TOK, (p + 1) * TOK)
        scores = mm(of_pair(p, keys), q_ref[i, :, cols], NT) * HEAD_DIM ** (-0.5)
        halves = []
        for h in range(2):
            s = jnp.where(seen, scores[h * TOK : (h + 1) * TOK], -1e30)
            e = jnp.exp(s - jnp.max(s, axis=0, keepdims=True))
            halves.append((e / jnp.sum(e, axis=0, keepdims=True)).astype(BF))
        pt = jnp.concatenate(halves, axis=0)
        pt_ref[i, p] = pt
        att_ref[:, cols] = mm(pt, of_pair(p, vals), TN).astype(BF)
    at_ref[:, columns] = att_ref[...].T
    return xf


def gather_kernel(
    x_ref, cot_ref, gain_ref, wq_ref, wkv_ref, wo_ref, wg_ref, wu_ref, wd_ref,
    cut_ref, allcot_ref, nt_ref, at_ref, q_ref, kv_ref, pt_ref, pg_ref, pu_ref, pd_ref,
    xs_ref, att_ref, send_m, recv_m, send_z, recv_z, send_w, recv_w,
):
    pos = places()
    entry_barrier([pos[k] for k in ("xp", "xm", "yp", "co", "zp", "zm", "lp")])
    lo, hi = pl.ds(0, HALF), pl.ds(HALF, HALF)

    def mem_copies(base, all_ref, own):
        plan = [
            (own, all_ref.at[1], "xp"),
            (own, all_ref.at[2], "xm"),
            (own, all_ref.at[4], "yp"),
            (all_ref.at[1, lo], all_ref.at[3, lo], "xp"),
            (all_ref.at[2, hi], all_ref.at[3, hi], "xm"),
            (all_ref.at[4], all_ref.at[5], "xp"),
            (all_ref.at[4], all_ref.at[6], "xm"),
            (all_ref.at[5, lo], all_ref.at[7, lo], "xp"),
            (all_ref.at[6, hi], all_ref.at[7, hi], "xm"),
        ]
        return [remote(s, d, send_m, recv_m, base + k, pos[n]) for k, (s, d, n) in enumerate(plan)]

    cot = mem_copies(0, allcot_ref, cot_ref)
    cut = mem_copies(9, cut_ref, cut_ref.at[0])

    ring = {}
    for stream in range(2):
        for way, name in ((0, "zp"), (1, "zm")):
            for step in range(1, 5):
                src = x_ref if stream == 0 else xs_ref.at[1]
                if step > 1:
                    src = xs_ref.at[ring_slot(step - 1, stream, way)]
                dst = xs_ref.at[ring_slot(step, stream, way)]
                if step == 4:
                    part = (lo, hi)[way]
                    src, dst = src.at[part], dst.at[part]
                k = 1 + (step - 1) * 4 + stream * 2 + way
                ring[step, stream, way] = remote(src, dst, send_z, recv_z, k, pos[name])
    across = remote(x_ref, xs_ref.at[1], send_z, recv_z, 0, pos["lp"])
    swap = [
        remote(s, d, send_w, recv_w, k, pos["co"])
        for k, (s, d) in enumerate(((wg_ref, pg_ref), (wu_ref, pu_ref), (wd_ref, pd_ref)))
    ]

    across.start()
    for copy in cot[:3] + [ring[1, 0, 0], ring[1, 0, 1]] + swap:
        copy.start()
    allcot_ref[0] = cot_ref[...]
    gain = gain_ref[...]
    saved = (nt_ref, at_ref, q_ref, kv_ref, pt_ref, att_ref)
    xf = client_forward(0, x_ref[...], gain, wq_ref, wkv_ref, *saved)
    cut_ref[0] = (xf + mm(att_ref[...], wo_ref[...])).astype(BF)
    for copy in cut[:3]:
        copy.start()

    def from_neighbours(copies):
        copies[0].wait_recv()
        copies[3].start()
        copies[1].wait_recv()
        copies[4].start()

    def from_across(copies):
        copies[2].wait_recv()
        copies[5].start()
        copies[6].start()

    def from_far(copies):
        copies[5].wait_recv()
        copies[7].start()
        copies[6].wait_recv()
        copies[8].start()

    def on_ring(step, stream):
        for way in range(2):
            ring[step, stream, way].wait_recv()
            if step < 4:
                ring[step + 1, stream, way].start()

    def first():
        across.wait_recv()
        ring[1, 1, 0].start()
        ring[1, 1, 1].start()
        from_neighbours(cot)
        from_across(cot)

    events = {
        1: [first],
        2: [lambda: on_ring(1, 0)],
        3: [lambda: from_neighbours(cut), lambda: from_across(cut)],
        4: [lambda: on_ring(1, 1)],
        5: [lambda: from_far(cot)],
        6: [lambda: on_ring(2, 0)],
        7: [lambda: from_far(cut)],
        8: [lambda: on_ring(2, 1)],
        10: [lambda: on_ring(3, 0)],
        12: [lambda: on_ring(3, 1)],
        14: [lambda: on_ring(4, 0)],
        15: [lambda: on_ring(4, 1)],
    }

    @pl.loop(1, 16)
    def _(i):
        for at, todo in events.items():
            @pl.when(i == at)
            def _():
                for act in todo:
                    act()

        client_forward(i, xs_ref[i], gain, wq_ref, wkv_ref, *saved)

    for copies in (cot, cut):
        for k in (3, 4, 7, 8):
            copies[k].wait_recv()
    for copy in swap:
        copy.wait_recv()
    for copy in cot + cut + list(ring.values()) + [across] + swap:
        copy.wait_send()


def gather_call(x, cot, gain, wq, wkv, wo, wg, wu, wd):
    vmem, anyspace = pl.BlockSpec(memory_space=pltpu.VMEM), pl.BlockSpec(memory_space=pl.ANY)
    sds = jax.ShapeDtypeStruct
    return pl.pallas_call(
        gather_kernel,
        out_shape=(
            sds((8, TOK, D), BF), sds((8, TOK, D), BF), sds((D, 16 * TOK), BF), sds((D, 16 * TOK), BF),
            sds((16, TOK, D), BF), sds((16, TOK, 2 * TOK), BF), sds((16, PAIRS, 2 * TOK, TOK), BF),
            sds(wg.shape, BF), sds(wu.shape, BF), sds(wd.shape, BF),
        ),
        in_specs=[vmem] * 6 + [anyspace] * 3,
        out_specs=[vmem] * 7 + [anyspace] * 3,
        scratch_shapes=[
            pltpu.VMEM((16, TOK, D), BF), pltpu.VMEM((TOK, D), BF),
            pltpu.SemaphoreType.DMA((18,)), pltpu.SemaphoreType.DMA((18,)),
            pltpu.SemaphoreType.DMA((17,)), pltpu.SemaphoreType.DMA((17,)),
            pltpu.SemaphoreType.DMA((3,)), pltpu.SemaphoreType.DMA((3,)),
        ],
        compiler_params=pltpu.CompilerParams(collective_id=0, has_side_effects=True, vmem_limit_bytes=56 * 2**20),
        name="gather_forward",
    )(x, cot, gain, wq, wkv, wo, wg, wu, wd)


def client_backward(i, cg, wo_ref, q_ref, kv_ref, pt_ref, dq_ref, dkv_ref, datt_ref):
    datt_ref[...] = mm(cg, wo_ref[...], NT).astype(BF)
    kv = kv_ref[i]
    keys, vals = stacked_heads(kv[:, :TOK]), stacked_heads(kv[:, TOK:])
    rows = pl.ds(pl.multiple_of(i * TOK, TOK), TOK)
    sums = {}

    def add(key, value):
        sums[key] = value if key not in sums else sums[key] + value

    for p in range(PAIRS):
        cols = slice(p * TOK, (p + 1) * TOK)
        d_out = datt_ref[:, cols]
        pt = pt_ref[i, p]
        d_probs = mm(of_pair(p, vals), d_out, NT)
        wide = pt.astype(F32)
        halves = []
        for h in range(2):
            half = slice(h * TOK, (h + 1) * TOK)
            both = d_probs[half] * wide[half]
            halves.append((both - wide[half] * jnp.sum(both, axis=0, keepdims=True)) * HEAD_DIM ** (-0.5))
        ds = jnp.concatenate(halves, axis=0).astype(BF)
        dq_ref[rows, cols] = mm(ds, of_pair(p, keys), TN).astype(BF)
        dk, dv = mm(ds, q_ref[i, :, cols]), mm(pt, d_out)
        for h in range(2):
            kv_head = (2 * p + h) // PAIRS
            half = slice(h * TOK, (h + 1) * TOK)
            add(("k", kv_head, h), dk[half])
            add(("v", kv_head, h), dv[half])
    low = lax.broadcasted_iota(jnp.int32, (TOK, TOK), 1) < HEAD_DIM
    for at, name in enumerate(("k", "v")):
        first = sums[name, 0, 0] + pltpu.roll(sums[name, 0, 1], HEAD_DIM, 1)
        second = sums[name, 1, 1] + pltpu.roll(sums[name, 1, 0], HEAD_DIM, 1)
        dkv_ref[rows, at * TOK : (at + 1) * TOK] = jnp.where(low, first, second).astype(BF)


def back_kernel(
    ls_ref, served_ref, cut_ref, og_ref, ou_ref, od_ref, nt_ref, at_ref, q_ref, kv_ref, pt_ref, wo_ref,
    out_ref, gq_ref, gkv_ref, go_ref, pg_ref, pu_ref, pd_ref,
    part_ref, mine_ref, slices_ref, cg_ref, got_ref, dq_ref, dkv_ref, datt_ref,
    send_r, recv_r, send_a, recv_a, send_z, recv_z, send_c, recv_c, send_s, recv_s, send_w, recv_w,
):
    pos = places()
    m, c = pos["m"], pos["c"]
    peers = [{"mem": (m + d) % 16} for d in range(1, 16)]
    entry_barrier(peers + [pos[k] for k in ("zp", "zm", "lp")])

    shares = [
        remote(ls_ref.at[(m + d) % 16], part_ref.at[d - 1], send_r, recv_r, d - 1, peers[d - 1]) for d in range(1, 16)
    ]
    for copy in shares:
        copy.start()
    total = ls_ref[m].astype(F32)
    for d in range(15):
        shares[d].wait_recv()
        total = total + part_ref[d].astype(F32)
    mine_ref[...] = (total * (1.0 / 16)).astype(BF)
    spread = [remote(mine_ref, slices_ref.at[m], send_a, recv_a, d, peers[d]) for d in range(15)]
    for copy in spread:
        copy.start()
    slices_ref[m] = mine_ref[...]
    for d in range(15):
        spread[d].wait_recv()
    cg_ref[0] = slices_ref[...].astype(F32).reshape(TOK, D).astype(BF)

    def part(slot, start, size):
        return cg_ref.at[slot, pl.ds(pl.multiple_of(c * HALF + start, 32), size)]

    ring, over = {}, {}
    for stream in range(2):
        for way, name in ((0, "zp"), (1, "zm")):
            for step in range(1, 5):
                before = stream if step == 1 else ring_slot(step - 1, stream, way)
                after = ring_slot(step, stream, way)
                span = (0, HALF) if step < 4 else (way * 32, 32)
                k = 1 + (step - 1) * 4 + stream * 2 + way
                ring[step, stream, way] = remote(part(before, *span), part(after, *span), send_z, recv_z, k, pos[name])
    across = remote(part(0, 0, HALF), part(1, 0, HALF), send_z, recv_z, 0, pos["lp"])
    for slot in range(1, 16):
        over[slot] = remote(part(slot, 0, HALF), part(slot, 0, HALF), send_c, recv_c, slot - 1, pos["co"])
    across.start()
    ring[1, 0, 0].start()
    ring[1, 0, 1].start()
    names = ("xm", "xp", "x2", "yp", "yxm", "yxp", "yx2")
    serve = [remote(served_ref.at[k + 1], got_ref.at[k], send_s, recv_s, k, pos[n]) for k, n in enumerate(names)]
    swap = [
        remote(s, d, send_w, recv_w, k, pos["co"])
        for k, (s, d) in enumerate(((og_ref, pg_ref), (ou_ref, pu_ref), (od_ref, pd_ref)))
    ]
    for copy in serve + swap:
        copy.start()

    def on_ring(step, stream):
        for way in range(2):
            ring[step, stream, way].wait_recv()
            if step < 4:
                ring[step + 1, stream, way].start()
                over[ring_slot(step, stream, way)].start()
        if step == 4:
            over[14 + stream].start()

    def first():
        across.wait_recv()
        ring[1, 1, 0].start()
        ring[1, 1, 1].start()
        over[1].start()
        on_ring(1, 0)
        over[1].wait_recv()

    def handed(*slots):
        for slot in slots:
            over[slot].wait_recv()

    events = {
        1: [first],
        2: [lambda: on_ring(1, 1), lambda: handed(2, 3)],
        4: [lambda: on_ring(2, 0), lambda: handed(4, 5)],
        6: [lambda: on_ring(2, 1), lambda: handed(6, 7)],
        8: [lambda: on_ring(3, 0), lambda: handed(8, 9)],
        10: [lambda: on_ring(3, 1), lambda: handed(10, 11)],
        12: [lambda: on_ring(4, 0), lambda: on_ring(4, 1), lambda: handed(12, 13)],
        14: [lambda: handed(14, 15)],
    }

    @pl.loop(0, 16)
    def _(i):
        for at, todo in events.items():
            @pl.when(i == at)
            def _():
                for act in todo:
                    act()

        client_backward(i, cg_ref[i], wo_ref, q_ref, kv_ref, pt_ref, dq_ref, dkv_ref, datt_ref)

    @pl.loop(0, 7)
    def _(t):
        rows = pl.ds(pl.multiple_of(t * TOK, TOK), TOK)
        gq_ref[rows, :] = (mm(nt_ref[rows, :], dq_ref[...]) * (1.0 / 16)).astype(BF)
        gkv_ref[rows, :] = (mm(nt_ref[rows, :], dkv_ref[...]) * (1.0 / 16)).astype(BF)
        go_ref[rows, :] = (mm(at_ref[rows, :], cg_ref[...].reshape(16 * TOK, D)) * (1.0 / 16)).astype(BF)

    for copy in serve:
        copy.wait_recv()
    out = cut_ref[...].astype(F32) + served_ref[0].astype(F32)
    for k in range(7):
        out = out + got_ref[k].astype(F32)
    out_ref[...] = out.astype(BF)
    for copy in swap:
        copy.wait_recv()
    for copy in shares + spread + list(ring.values()) + [across] + list(over.values()) + serve + swap:
        copy.wait_send()


def back_call(ls, served, cut, og, ou, od, nt, at, q, kv, pt, wo):
    vmem, anyspace = pl.BlockSpec(memory_space=pltpu.VMEM), pl.BlockSpec(memory_space=pl.ANY)
    sds = jax.ShapeDtypeStruct
    sem = pltpu.SemaphoreType.DMA
    return pl.pallas_call(
        back_kernel,
        out_shape=(
            sds((TOK, D), BF), sds((D, D), BF), sds((D, 2 * TOK), BF), sds((D, D), BF),
            sds(og.shape, BF), sds(ou.shape, BF), sds(od.shape, BF),
        ),
        in_specs=[vmem] * 3 + [anyspace] * 3 + [vmem] * 6,
        out_specs=[vmem] * 4 + [anyspace] * 3,
        scratch_shapes=[
            pltpu.VMEM((15, 8, D), BF), pltpu.VMEM((8, D), BF), pltpu.VMEM((16, 8, D), BF),
            pltpu.VMEM((16, TOK, D), BF), pltpu.VMEM((7, TOK, D), BF),
            pltpu.VMEM((16 * TOK, D), BF), pltpu.VMEM((16 * TOK, 2 * TOK), BF), pltpu.VMEM((TOK, D), BF),
            sem((15,)), sem((15,)), sem((15,)), sem((15,)), sem((17,)), sem((17,)), sem((15,)), sem((15,)),
            sem((7,)), sem((7,)), sem((3,)), sem((3,)),
        ],
        compiler_params=pltpu.CompilerParams(collective_id=1, has_side_effects=True, vmem_limit_bytes=56 * 2**20),
        name="cut_grad_backward",
    )(ls, served, cut, og, ou, od, nt, at, q, kv, pt, wo)


def server(cuts, cots, s_gain, gate_w, up_w, down_w):
    rows = cuts.reshape(-1, D)
    cot = cots.reshape(-1, D)
    h_float = rows.astype(F32)
    inv_rms = lax.rsqrt(jnp.mean(h_float * h_float, axis=-1, keepdims=True) + EPS)
    normed = (h_float * inv_rms * s_gain).astype(BF)
    gate_act, up_act = mm(normed, gate_w), mm(normed, up_w)
    sigma = jax.nn.sigmoid(gate_act)
    hidden = (gate_act * sigma * up_act).astype(BF)
    served = mm(hidden, down_w).astype(BF).reshape(cuts.shape)
    d_hidden = mm(cot, down_w, NT)
    d_gate = (d_hidden * up_act * sigma * (1.0 + gate_act * (1.0 - sigma))).astype(BF)
    d_up = (d_hidden * gate_act * sigma).astype(BF)
    d_normed = mm(d_gate, gate_w, NT) + mm(d_up, up_w, NT)
    scaled = d_normed * s_gain
    pushed = inv_rms * scaled - h_float * inv_rms**3 * jnp.mean(scaled * h_float, axis=-1, keepdims=True)
    local_sum = jnp.sum(pushed.reshape(cuts.shape), axis=0) + cots[0].astype(F32)
    return served, local_sum.astype(BF), mm(normed, d_gate, TN), mm(normed, d_up, TN), mm(hidden, cot, TN)


def on_device(
    client_input, client_gain, w_query, w_keyval, w_out, server_gain, w_gate, w_up, w_down, out_grad, valid
):
    live = jnp.arange(TOK) < valid[0, 0]
    cot = jnp.where(live[:, None], out_grad[0, 0], jnp.zeros_like(out_grad[0, 0]))
    gate_w, up_w, down_w = w_gate[0], w_up[0], w_down[0]
    width = gate_w.shape[1]
    cuts, cots, nt, at, q, kv, pt, far_gate, far_up, far_down = gather_call(
        client_input[0, 0], cot, client_gain, w_query[0], w_keyval[0], w_out[0], gate_w, up_w, down_w
    )
    served, local_sum, gg, gu, gd = server(
        cuts,
        cots,
        server_gain[0],
        jnp.concatenate([gate_w, far_gate], axis=1),
        jnp.concatenate([up_w, far_up], axis=1),
        jnp.concatenate([down_w, far_down], axis=0),
    )
    server_out, grad_q, grad_kv, grad_o, rg, ru, rd = back_call(
        local_sum.reshape(16, 8, D),
        served,
        cuts[0],
        gg[:, width:].astype(BF),
        gu[:, width:].astype(BF),
        gd[width:].astype(BF),
        nt, at, q, kv, pt, w_out[0],
    )
    join = lambda own, got: (own + got.astype(F32)).astype(BF)[None]
    return (
        server_out[None, None],
        grad_q[None],
        grad_kv[None],
        grad_o[None],
        join(gg[:, :width], rg),
        join(gu[:, :width], ru),
        join(gd[:width], rd),
    )


def solution(mesh):
    in_specs = (
        P("grp", "mem", None, None),
        P("mem", None),
        P("mem", None, None),
        P("mem", None, None),
        P("mem", None, None),
        P("grp", None),
        P("grp", None, "mem"),
        P("grp", None, "mem"),
        P("grp", "mem", None),
        P("grp", "mem", None, None),
        P("grp", "mem"),
    )
    out_specs = (
        P("grp", "mem", None, None),
        P("mem", None, None),
        P("mem", None, None),
        P("mem", None, None),
        P("grp", None, "mem"),
        P("grp", None, "mem"),
        P("grp", "mem", None),
    )
    return jax.shard_map(
        on_device, mesh=mesh, in_specs=in_specs, out_specs=out_specs, check_vma=False
    )
```

```python
import functools

import jax
import jax.numpy as jnp
from jax import lax
from jax.experimental import pallas as pl
from jax.experimental.pallas import tpu as pltpu
from jax.sharding import PartitionSpec as P

EPS = 1e-06
HEAD_DIM = 64
TOK = 128
D = 896
PAIRS = 7
BF = jnp.bfloat16
F32 = jnp.float32
MESH = pl.DeviceIdType.MESH
NN = (((1,), (0,)), ((), ()))
NT = (((1,), (1,)), ((), ()))
TN = (((0,), (0,)), ((), ()))
HALF = TOK // 2
SCALE = HEAD_DIM ** (-0.5)


def mm(a, b, dims=NN):
    return lax.dot_general(a, b, dims, preferred_element_type=F32)


def places():
    g, m = lax.axis_index("grp"), lax.axis_index("mem")
    l, z = g // 8, g % 8
    yh, x, c = m // 8, (m // 2) % 4, m % 2
    at = lambda y_, x_, c_: {"mem": y_ * 8 + x_ * 2 + c_}
    return dict(
        m=m,
        c=c,
        xp=at(yh, (x + 1) % 4, c),
        xm=at(yh, (x + 3) % 4, c),
        x2=at(yh, (x + 2) % 4, c),
        yp=at(1 - yh, x, c),
        yxp=at(1 - yh, (x + 1) % 4, c),
        yxm=at(1 - yh, (x + 3) % 4, c),
        yx2=at(1 - yh, (x + 2) % 4, c),
        co=at(yh, x, 1 - c),
        zp={"grp": l * 8 + (z + 1) % 8},
        zm={"grp": l * 8 + (z + 7) % 8},
        lp={"grp": (1 - l) * 8 + z},
    )


def remote(src, dst, send, recv, k, device):
    return pltpu.make_async_remote_copy(
        src_ref=src, dst_ref=dst, send_sem=send.at[k], recv_sem=recv.at[k], device_id=device, device_id_type=MESH
    )


def entry_barrier(devices):
    barrier = pltpu.get_barrier_semaphore()
    for device in devices:
        pl.semaphore_signal(barrier, inc=1, device_id=device, device_id_type=MESH)
    pl.semaphore_wait(barrier, len(devices))


def ring_slot(step, stream, way):
    return 2 + 4 * (step - 1) + 2 * stream + way if step < 4 else 14 + stream


def stacked_heads(both):
    wide = both.astype(F32)
    turned = pltpu.roll(wide, HEAD_DIM, 1)
    low = lax.broadcasted_iota(jnp.int32, wide.shape, 1) < HEAD_DIM
    zero = jnp.zeros_like(wide)
    first0, second0 = jnp.where(low, wide, zero), jnp.where(low, zero, turned)
    first1, second1 = jnp.where(low, turned, zero), jnp.where(low, zero, wide)
    pair = lambda a, b: jnp.concatenate([a, b], axis=0).astype(BF)
    return pair(first0, second0), pair(first0, second1), pair(first1, second1)


def of_pair(p, three):
    return three[0] if p < 3 else three[1] if p == 3 else three[2]


def forward_clients(slot, count, xs_ref, gain, wq_ref, wkv_ref, nt_ref, at_ref, q_ref, kv_ref, pt_ref, att_ref):
    size = count * TOK
    xf = xs_ref[pl.ds(slot, count)].reshape(size, D).astype(F32)
    inv = lax.rsqrt(jnp.mean(xf * xf, axis=-1, keepdims=True) + EPS)
    normed = (xf * inv * gain).astype(BF)
    columns = pl.ds(pl.multiple_of(slot * TOK, TOK), size)
    nt_ref[:, columns] = normed.T
    q_ref[pl.ds(slot, count)] = mm(normed, wq_ref[...]).astype(BF).reshape(count, TOK, D)
    kv = mm(normed, wkv_ref[...]).astype(BF)
    kv_ref[pl.ds(slot, count)] = kv.reshape(count, TOK, 2 * TOK)
    split = [kv[n * TOK : (n + 1) * TOK] for n in range(count)]
    keys = [stacked_heads(s[:, :TOK]) for s in split]
    vals = [stacked_heads(s[:, TOK:]) for s in split]
    s_at = lax.broadcasted_iota(jnp.int32, (TOK, TOK), 0)
    t_at = lax.broadcasted_iota(jnp.int32, (TOK, TOK), 1)
    seen = s_at <= t_at
    for p in range(PAIRS):
        cols = slice(p * TOK, (p + 1) * TOK)
        for n in range(count):
            scores = mm(of_pair(p, keys[n]), q_ref[slot + n, :, cols], NT) * SCALE
            halves = []
            for h in range(2):
                s = jnp.where(seen, scores[h * TOK : (h + 1) * TOK], -1e30)
                e = jnp.exp(s - jnp.max(s, axis=0, keepdims=True))
                halves.append((e * (1.0 / jnp.sum(e, axis=0, keepdims=True))).astype(BF))
            pt = jnp.concatenate(halves, axis=0)
            pt_ref[slot + n, p] = pt
            att_ref[n * TOK : (n + 1) * TOK, cols] = mm(pt, of_pair(p, vals[n]), TN).astype(BF)
    at_ref[:, columns] = att_ref[:size, :].T
    return xf


def backward_clients(slot, count, cg_ref, wo_ref, q_ref, kv_ref, pt_ref, dq_ref, dkv_ref, datt_ref):
    size = count * TOK
    datt_ref[:size, :] = mm(cg_ref[pl.ds(slot, count)].reshape(size, D), wo_ref[...], NT).astype(BF)
    split = [kv_ref[slot + n] for n in range(count)]
    keys = [stacked_heads(s[:, :TOK]) for s in split]
    vals = [stacked_heads(s[:, TOK:]) for s in split]
    sums = {}

    def add(key, value):
        sums[key] = value if key not in sums else sums[key] + value

    for p in range(PAIRS):
        cols = slice(p * TOK, (p + 1) * TOK)
        for n in range(count):
            d_out = datt_ref[n * TOK : (n + 1) * TOK, cols]
            pt = pt_ref[slot + n, p]
            d_probs = mm(of_pair(p, vals[n]), d_out, NT)
            wide = pt.astype(F32)
            halves = []
            for h in range(2):
                half = slice(h * TOK, (h + 1) * TOK)
                both = d_probs[half] * wide[half]
                halves.append((both - wide[half] * jnp.sum(both, axis=0, keepdims=True)) * SCALE)
            ds = jnp.concatenate(halves, axis=0).astype(BF)
            dq_ref[slot + n, :, cols] = mm(ds, of_pair(p, keys[n]), TN).astype(BF)
            dk, dv = mm(ds, q_ref[slot + n, :, cols]), mm(pt, d_out)
            for h in range(2):
                kv_head = (2 * p + h) // PAIRS
                half = slice(h * TOK, (h + 1) * TOK)
                add((n, "k", kv_head, h), dk[half])
                add((n, "v", kv_head, h), dv[half])
    low = lax.broadcasted_iota(jnp.int32, (TOK, TOK), 1) < HEAD_DIM
    for n in range(count):
        for at, name in enumerate(("k", "v")):
            first = sums[n, name, 0, 0] + pltpu.roll(sums[n, name, 0, 1], HEAD_DIM, 1)
            second = sums[n, name, 1, 1] + pltpu.roll(sums[n, name, 1, 0], HEAD_DIM, 1)
            dkv_ref[slot + n, :, at * TOK : (at + 1) * TOK] = jnp.where(low, first, second).astype(BF)


def last_products(left_ref, pairs):
    step = D // 4

    @pl.loop(0, 4)
    def _(t):
        rows = pl.ds(pl.multiple_of(t * step, step), step)
        for right_ref, out_ref in pairs:
            right = right_ref[...].reshape(16 * TOK, right_ref.shape[-1])
            out_ref[rows, :] = (mm(left_ref[rows, :], right) * (1.0 / 16)).astype(BF)


def server_layer(mc_ref, sgain, ws_ref, served_ref, ls_ref, gr_ref, ns_ref, act_ref, sum_ref):
    size = 2 * TOK
    sum_ref[...] = mc_ref[8].astype(F32)

    @pl.loop(0, 4)
    def _(j):
        hf = mc_ref[pl.ds(2 * j, 2)].reshape(size, D).astype(F32)
        cot = mc_ref[pl.ds(8 + 2 * j, 2)].reshape(size, D)
        inv = lax.rsqrt(jnp.mean(hf * hf, axis=-1, keepdims=True) + EPS)
        normed = (hf * inv * sgain).astype(BF)
        ns_ref[pl.ds(pl.multiple_of(j * size, size), size), :] = normed
        gate, up = mm(ws_ref[0], normed, NT), mm(ws_ref[1], normed, NT)
        d_hidden = mm(ws_ref[2], cot, NT)
        sigma = jax.nn.sigmoid(gate)
        silu = gate * sigma
        hidden = (silu * up).astype(BF)
        d_gate = (d_hidden * up * sigma * (1.0 + gate * (1.0 - sigma))).astype(BF)
        d_up = (d_hidden * silu).astype(BF)
        columns = pl.ds(pl.multiple_of(j * size, size), size)
        act_ref[0, :, columns] = d_gate
        act_ref[1, :, columns] = d_up
        act_ref[2, :, columns] = hidden
        served_ref[pl.ds(2 * j, 2)] = mm(hidden, ws_ref[2], TN).astype(BF).reshape(2, TOK, D)
        scaled = (mm(d_gate, ws_ref[0], TN) + mm(d_up, ws_ref[1], TN)) * sgain
        pushed = inv * scaled - hf * (inv * inv * inv) * jnp.mean(scaled * hf, axis=-1, keepdims=True)
        sum_ref[...] += pushed[:TOK] + pushed[TOK:]

    ls_ref[...] = sum_ref[...].reshape(16, 8, D).astype(BF)


def server_gradients(mc_ref, gr_ref, ns_ref, act_ref):
    width = gr_ref.shape[1] // 2

    @pl.loop(0, 2)
    def _(t):
        rows = pl.ds(pl.multiple_of(t * width, 16), width)
        gr_ref[0, rows, :] = mm(act_ref[0, rows, :], ns_ref[...]).astype(BF)
        gr_ref[1, rows, :] = mm(act_ref[1, rows, :], ns_ref[...]).astype(BF)
        gr_ref[2, rows, :] = mm(act_ref[2, rows, :], mc_ref[pl.ds(8, 8)].reshape(8 * TOK, D)).astype(BF)


def step_kernel(
    valid_ref, x_ref, cot_ref, gain_ref, sgain_ref, wq_hbm, wkv_hbm, wo_hbm, wg_hbm, wu_hbm, wd_hbm,
    out_ref, gq_hbm, gkv_hbm, go_hbm, own_hbm, got_hbm,
    wq_ref, wkv_ref, wo_ref, ws_ref, xs_ref, mc_ref, nt_ref, at_ref, q_ref, kv_ref, pt_ref, att_ref,
    served_ref, gr_ref, ns_ref, act_ref, sum_ref, ls_ref, part_ref, mine_ref, slices_ref, cg_ref, back_ref, dkv_ref,
    load, send_m, recv_m, send_x, recv_x, send_w, recv_w, send_r, recv_r, send_a, recv_a,
    send_z, recv_z, send_c, recv_c, send_s, recv_s, send_g, recv_g, keep,
):
    pos = places()
    m, c = pos["m"], pos["c"]
    width = wg_hbm.shape[0]
    near, far = pl.ds(0, width), pl.ds(width, width)
    weights = (wg_hbm, wu_hbm, wd_hbm)
    loads = [
        pltpu.make_async_copy(s, d, load.at[k])
        for k, (s, d) in enumerate(
            [(wq_hbm, wq_ref), (wkv_hbm, wkv_ref), (wo_hbm, wo_ref)]
            + [(w, ws_ref.at[k, near]) for k, w in enumerate(weights)]
        )
    ]
    for copy in loads:
        copy.start()
    live = lax.broadcasted_iota(jnp.int32, (TOK, D), 0) < valid_ref[0, 0]
    mc_ref[8] = jnp.where(live, cot_ref[...].astype(F32), 0.0).astype(BF)
    xs_ref[0] = x_ref[...]

    peers = [{"mem": (m + d) % 16} for d in range(1, 16)]
    entry_barrier(peers + [pos[k] for k in ("zp", "zm", "lp")])
    lo, hi = pl.ds(0, HALF), pl.ds(HALF, HALF)

    def mem_copies(sems, base):
        at = lambda k: mc_ref.at[base + k]
        plan = [
            (at(0), at(1), "xp"),
            (at(0), at(2), "xm"),
            (at(0), at(4), "yp"),
            (mc_ref.at[base + 1, lo], mc_ref.at[base + 3, lo], "xp"),
            (mc_ref.at[base + 2, hi], mc_ref.at[base + 3, hi], "xm"),
            (at(4), at(5), "xp"),
            (at(4), at(6), "xm"),
            (mc_ref.at[base + 5, lo], mc_ref.at[base + 7, lo], "xp"),
            (mc_ref.at[base + 6, hi], mc_ref.at[base + 7, hi], "xm"),
        ]
        return [remote(s, d, send_m, recv_m, sems + k, pos[n]) for k, (s, d, n) in enumerate(plan)]

    cot, cut = mem_copies(0, 8), mem_copies(9, 0)

    def ring_copies(first, block, send, recv):
        ring = {}
        for stream in range(2):
            for way, name in ((0, "zp"), (1, "zm")):
                for step in range(1, 5):
                    before = stream if step == 1 else ring_slot(step - 1, stream, way)
                    after = ring_slot(step, stream, way)
                    src = first if before == 0 else block(before, step == 4, way)
                    k = 1 + (step - 1) * 4 + stream * 2 + way
                    ring[step, stream, way] = remote(src, block(after, step == 4, way), send, recv, k, pos[name])
        return remote(first, block(1, False, 0), send, recv, 0, pos["lp"]), ring

    def input_block(slot, halved, way):
        return xs_ref.at[slot, (lo, hi)[way]] if halved else xs_ref.at[slot]

    in_across, in_ring = ring_copies(x_ref, input_block, send_x, recv_x)
    swap = [remote(w, ws_ref.at[k, far], send_w, recv_w, k, pos["co"]) for k, w in enumerate(weights)]

    def grad_block(slot, halved, way):
        start, size = (way * 32, 32) if halved else (0, HALF)
        return cg_ref.at[slot, pl.ds(pl.multiple_of(c * HALF + start, 32), size)]

    cg_across, cg_ring = ring_copies(grad_block(0, False, 0), grad_block, send_z, recv_z)
    over = {
        slot: remote(grad_block(slot, False, 0), grad_block(slot, False, 0), send_c, recv_c, slot - 1, pos["co"])
        for slot in range(1, 16)
    }
    shares = [remote(ls_ref.at[(m + d) % 16], part_ref.at[d - 1], send_r, recv_r, d - 1, peers[d - 1]) for d in range(1, 16)]
    spread = [remote(mine_ref, slices_ref.at[m], send_a, recv_a, d, peers[d]) for d in range(15)]
    names = ("xm", "xp", "x2", "yp", "yxm", "yxp", "yx2")
    serve = [remote(served_ref.at[k + 1], back_ref.at[k], send_s, recv_s, k, pos[n]) for k, n in enumerate(names)]
    trade = [remote(gr_ref.at[k, far], got_hbm.at[k], send_g, recv_g, k, pos["co"]) for k in range(3)]
    keeps = [pltpu.make_async_copy(gr_ref.at[k, near], own_hbm.at[k], keep.at[k]) for k in range(3)]

    for copy in [in_across] + cot[:3] + [in_ring[1, 0, 0], in_ring[1, 0, 1]] + swap:
        copy.start()
    gain, sgain = gain_ref[...], sgain_ref[...]
    for copy in loads[:3]:
        copy.wait()
    saved = (nt_ref, at_ref, q_ref, kv_ref, pt_ref, att_ref)
    xf = forward_clients(0, 1, xs_ref, gain, wq_ref, wkv_ref, *saved)
    mc_ref[0] = (xf + mm(att_ref[:TOK, :], wo_ref[...])).astype(BF)
    for copy in cut[:3]:
        copy.start()

    def from_neighbours(copies):
        copies[0].wait_recv()
        copies[3].start()
        copies[1].wait_recv()
        copies[4].start()

    def from_across(copies):
        copies[2].wait_recv()
        copies[5].start()
        copies[6].start()

    def from_far(copies):
        copies[5].wait_recv()
        copies[7].start()
        copies[6].wait_recv()
        copies[8].start()

    def inputs(step, stream):
        for way in range(2):
            in_ring[step, stream, way].wait_recv()
            if step < 4:
                in_ring[step + 1, stream, way].start()

    def first_inputs():
        in_across.wait_recv()
        in_ring[1, 1, 0].start()
        in_ring[1, 1, 1].start()

    def server():
        for copies in (cot, cut):
            for k in (3, 4, 7, 8):
                copies[k].wait_recv()
        for copy in loads[3:]:
            copy.wait()
        for copy in swap:
            copy.wait_recv()
        server_layer(mc_ref, sgain, ws_ref, served_ref, ls_ref, gr_ref, ns_ref, act_ref, sum_ref)
        for copy in shares:
            copy.start()

    def gradients():
        server_gradients(mc_ref, gr_ref, ns_ref, act_ref)
        sum_ref[...] = mc_ref[0].astype(F32)

    def reduce():
        total = ls_ref[m].astype(F32)
        for d in range(15):
            shares[d].wait_recv()
            total = total + part_ref[d].astype(F32)
        mine_ref[...] = (total * (1.0 / 16)).astype(BF)
        for copy in spread:
            copy.start()
        slices_ref[m] = mine_ref[...]

    def own_group():
        for d in range(15):
            spread[d].wait_recv()
        cg_ref[0] = slices_ref[...].astype(F32).reshape(TOK, D).astype(BF)
        for copy in [cg_across, cg_ring[1, 0, 0], cg_ring[1, 0, 1]] + serve + trade + keeps:
            copy.start()

    def when_at(i, events):
        for at, todo in events.items():
            @pl.when(i == at)
            def _():
                for act in todo:
                    act()

    forward_events = {
        0: [first_inputs, lambda: from_neighbours(cot), lambda: from_across(cot)],
        1: [lambda: inputs(1, 0), lambda: from_neighbours(cut), lambda: from_across(cut)],
        2: [lambda: inputs(1, 1), lambda: from_far(cot)],
        3: [lambda: inputs(2, 0), lambda: from_far(cut)],
        4: [lambda: inputs(2, 1)],
        5: [server, lambda: inputs(3, 0), gradients],
        6: [reduce, lambda: inputs(3, 1)],
        7: [lambda: inputs(4, 0), lambda: inputs(4, 1), own_group],
    }

    @pl.loop(0, 8)
    def _(j):
        when_at(j, forward_events)
        forward_clients(2 * j, 2, xs_ref, gain, wq_ref, wkv_ref, *saved)

    def grads(step, stream):
        for way in range(2):
            cg_ring[step, stream, way].wait_recv()
            if step < 4:
                cg_ring[step + 1, stream, way].start()
                over[ring_slot(step, stream, way)].start()
        if step == 4:
            over[14 + stream].start()

    def first_grads():
        cg_across.wait_recv()
        cg_ring[1, 1, 0].start()
        cg_ring[1, 1, 1].start()
        over[1].start()

    def handed(*slots):
        for slot in slots:
            over[slot].wait_recv()

    for copy in cot + cut:
        copy.wait_send()
    backward_events = {
        0: [first_grads, lambda: grads(1, 0), lambda: handed(1)],
        1: [lambda: grads(1, 1), lambda: handed(2, 3)],
        2: [lambda: grads(2, 0), lambda: handed(4, 5)],
        3: [lambda: grads(2, 1), lambda: handed(6, 7)],
        4: [lambda: grads(3, 0), lambda: handed(8, 9)],
        5: [lambda: grads(3, 1), lambda: handed(10, 11)],
        6: [lambda: grads(4, 0), lambda: grads(4, 1), lambda: handed(12, 13)],
        7: [lambda: handed(14, 15)],
    }

    @pl.loop(0, 8)
    def _(j):
        when_at(j, backward_events)
        backward_clients(2 * j, 2, cg_ref, wo_ref, q_ref, kv_ref, pt_ref, mc_ref, dkv_ref, att_ref)

    go_ref = ns_ref.at[pl.ds(0, D)]
    done = [
        pltpu.make_async_copy(s, d, load.at[k])
        for k, (s, d) in enumerate([(go_ref, go_hbm), (wq_ref, gq_hbm), (wkv_ref, gkv_hbm)])
    ]
    last_products(at_ref, [(cg_ref, go_ref)])
    done[0].start()
    last_products(nt_ref, [(mc_ref, wq_ref), (dkv_ref, wkv_ref)])
    done[1].start()
    done[2].start()

    for copy in serve:
        copy.wait_recv()
    out = sum_ref[...] + served_ref[0].astype(F32)
    for k in range(7):
        out = out + back_ref[k].astype(F32)
    out_ref[...] = out.astype(BF)
    for copy in trade:
        copy.wait_recv()
    for copy in keeps + done:
        copy.wait()
    for copy in [in_across, cg_across] + list(in_ring.values()) + list(cg_ring.values()) + list(over.values()):
        copy.wait_send()
    for copy in swap + shares + spread + serve + trade:
        copy.wait_send()


def step_call(valid, x, cot, gain, sgain, wq, wkv, wo, wg, wu, wd):
    vmem, anyspace = pl.BlockSpec(memory_space=pltpu.VMEM), pl.BlockSpec(memory_space=pl.ANY)
    sds = jax.ShapeDtypeStruct
    sem = pltpu.SemaphoreType.DMA
    width = wg.shape[0]
    units = 2 * width
    block = pltpu.VMEM((TOK, D), BF)
    blocks = lambda n: pltpu.VMEM((n, TOK, D), BF)
    return pl.pallas_call(
        step_kernel,
        out_shape=(
            sds((TOK, D), BF), sds((D, D), BF), sds((D, 2 * TOK), BF), sds((D, D), BF),
            sds((3, width, D), BF), sds((3, width, D), BF),
        ),
        in_specs=[pl.BlockSpec(memory_space=pltpu.SMEM)] + [vmem] * 4 + [anyspace] * 6,
        out_specs=[vmem] + [anyspace] * 5,
        scratch_shapes=[
            pltpu.VMEM((D, D), BF), pltpu.VMEM((D, 2 * TOK), BF), pltpu.VMEM((D, D), BF), pltpu.VMEM((3, units, D), BF),
            blocks(16), blocks(16), pltpu.VMEM((D, 16 * TOK), BF), pltpu.VMEM((D, 16 * TOK), BF),
            blocks(16), pltpu.VMEM((16, TOK, 2 * TOK), BF), pltpu.VMEM((16, PAIRS, 2 * TOK, TOK), BF),
            pltpu.VMEM((2 * TOK, D), BF),
            blocks(8), pltpu.VMEM((3, units, D), BF), pltpu.VMEM((8 * TOK, D), BF), pltpu.VMEM((3, units, 8 * TOK), BF),
            pltpu.VMEM((TOK, D), F32), pltpu.VMEM((16, 8, D), BF), pltpu.VMEM((15, 8, D), BF), pltpu.VMEM((8, D), BF),
            pltpu.VMEM((16, 8, D), BF), blocks(16), blocks(7), pltpu.VMEM((16, TOK, 2 * TOK), BF),
            sem((6,)), sem((18,)), sem((18,)), sem((17,)), sem((17,)), sem((3,)), sem((3,)), sem((15,)), sem((15,)),
            sem((15,)), sem((15,)), sem((17,)), sem((17,)), sem((15,)), sem((15,)), sem((7,)), sem((7,)),
            sem((3,)), sem((3,)), sem((3,)),
        ],
        compiler_params=pltpu.CompilerParams(collective_id=0, has_side_effects=True, vmem_limit_bytes=60 * 1024 * 2**10),
        name="split_step",
    )(valid, x, cot, gain, sgain, wq, wkv, wo, wg, wu, wd)


def on_device(
    client_input, client_gain, w_query, w_keyval, w_out, server_gain, w_gate, w_up, w_down, out_grad, valid
):
    server_out, grad_q, grad_kv, grad_o, own, got = step_call(
        valid, client_input[0, 0], out_grad[0, 0], client_gain, server_gain, w_query[0], w_keyval[0], w_out[0],
        w_gate[0].T, w_up[0].T, w_down[0],
    )
    joined = (own.astype(F32) + got.astype(F32)).astype(BF)
    return (
        server_out[None, None],
        grad_q[None],
        grad_kv[None],
        grad_o[None],
        joined[0].T[None],
        joined[1].T[None],
        joined[2][None],
    )


def solution(mesh):
    in_specs = (
        P("grp", "mem", None, None),
        P("mem", None),
        P("mem", None, None),
        P("mem", None, None),
        P("mem", None, None),
        P("grp", None),
        P("grp", None, "mem"),
        P("grp", None, "mem"),
        P("grp", "mem", None),
        P("grp", "mem", None, None),
        P("grp", "mem"),
    )
    out_specs = (
        P("grp", "mem", None, None),
        P("mem", None, None),
        P("mem", None, None),
        P("mem", None, None),
        P("grp", None, "mem"),
        P("grp", None, "mem"),
        P("grp", "mem", None),
    )
    return jax.shard_map(
        on_device, mesh=mesh, in_specs=in_specs, out_specs=out_specs, check_vma=False
    )
```

```python
import functools

import jax
import jax.numpy as jnp
from jax import lax
from jax.experimental import pallas as pl
from jax.experimental.pallas import tpu as pltpu
from jax.sharding import PartitionSpec as P

EPS = 1e-06
HEAD_DIM = 64
TOK = 128
D = 896
PAIRS = 7
BF = jnp.bfloat16
F32 = jnp.float32
MESH = pl.DeviceIdType.MESH
NN = (((1,), (0,)), ((), ()))
NT = (((1,), (1,)), ((), ()))
TN = (((0,), (0,)), ((), ()))
HALF = TOK // 2
SCALE = HEAD_DIM ** (-0.5)


def mm(a, b, dims=NN):
    return lax.dot_general(a, b, dims, preferred_element_type=F32)


def places():
    g, m = lax.axis_index("grp"), lax.axis_index("mem")
    l, z = g // 8, g % 8
    yh, x, c = m // 8, (m // 2) % 4, m % 2
    at = lambda y_, x_, c_: {"mem": y_ * 8 + x_ * 2 + c_}
    return dict(
        m=m,
        c=c,
        xp=at(yh, (x + 1) % 4, c),
        xm=at(yh, (x + 3) % 4, c),
        x2=at(yh, (x + 2) % 4, c),
        yp=at(1 - yh, x, c),
        yxp=at(1 - yh, (x + 1) % 4, c),
        yxm=at(1 - yh, (x + 3) % 4, c),
        yx2=at(1 - yh, (x + 2) % 4, c),
        co=at(yh, x, 1 - c),
        zp={"grp": l * 8 + (z + 1) % 8},
        zm={"grp": l * 8 + (z + 7) % 8},
        lp={"grp": (1 - l) * 8 + z},
    )


def remote(src, dst, send, recv, k, device):
    return pltpu.make_async_remote_copy(
        src_ref=src, dst_ref=dst, send_sem=send.at[k], recv_sem=recv.at[k], device_id=device, device_id_type=MESH
    )


def entry_barrier(devices):
    barrier = pltpu.get_barrier_semaphore()
    for device in devices:
        pl.semaphore_signal(barrier, inc=1, device_id=device, device_id_type=MESH)
    pl.semaphore_wait(barrier, len(devices))


def ring_slot(step, stream, way):
    return 2 + 4 * (step - 1) + 2 * stream + way if step < 4 else 14 + stream


MEETS = (((0, 4), (4, 7)), ((0, 3), (3, 7)))
GROUPS = ((0, 3), (3, 4), (4, 7))


def head_rows(both):
    wide = both.astype(F32)
    turned = pltpu.roll(wide, HEAD_DIM, 1)
    low = lax.broadcasted_iota(jnp.int32, wide.shape, 1) < HEAD_DIM
    zero = jnp.zeros_like(wide)
    first = (jnp.where(low, wide, zero).astype(BF), jnp.where(low, turned, zero).astype(BF))
    second = (jnp.where(low, zero, turned).astype(BF), jnp.where(low, zero, wide).astype(BF))
    return first, second


def head_columns(both):
    turned = both.T
    zero = jnp.zeros((HEAD_DIM, TOK), BF)
    heads = (turned[:HEAD_DIM], turned[HEAD_DIM:])
    build = lambda a, b: jnp.concatenate(
        [jnp.concatenate([heads[a], zero], axis=1), jnp.concatenate([zero, heads[b]], axis=1)], axis=0
    )
    return build(0, 0), build(0, 1), build(1, 1)


def lanes(span):
    return slice(span[0] * TOK, span[1] * TOK)


def stack(ref, n, span):
    return ref[n, span[0] : span[1]].reshape((span[1] - span[0]) * TOK, TOK)


def forward_clients(slot, count, xs_ref, gain, wq_ref, wkv_ref, nt_ref, at_ref, q_ref, kv_ref, pt_ref):
    size = count * TOK
    xf = xs_ref[pl.ds(slot, count)].reshape(size, D).astype(F32)
    inv = lax.rsqrt(jnp.mean(xf * xf, axis=-1, keepdims=True) + EPS)
    normed = (xf * inv * gain).astype(BF)
    columns = pl.ds(pl.multiple_of(slot * TOK, TOK), size)
    nt_ref[:, columns] = normed.T
    queries = mm(normed, wq_ref[...]).astype(BF)
    kv = mm(normed, wkv_ref[...]).astype(BF)
    kv_ref[pl.ds(slot, count)] = kv.reshape(count, TOK, 2 * TOK)
    for n in range(count):
        for p in range(PAIRS):
            q_ref[slot + n, p] = queries[n * TOK : (n + 1) * TOK, lanes((p, p + 1))]
    s_at = lax.broadcasted_iota(jnp.int32, (TOK, TOK), 0)
    t_at = lax.broadcasted_iota(jnp.int32, (TOK, TOK), 1)
    seen = s_at <= t_at
    for place in range(2):
        for head in range(2):
            span = MEETS[place][head]
            for n in range(count):
                keys = head_rows(kv[n * TOK : (n + 1) * TOK, :TOK])
                scores = mm(keys[place][head], stack(q_ref, slot + n, span), NT) * SCALE
                for p in range(*span):
                    s = jnp.where(seen, scores[:, lanes((p - span[0], p - span[0] + 1))], -1e30)
                    e = jnp.exp(s - jnp.max(s, axis=0, keepdims=True))
                    pt = (e * (1.0 / jnp.sum(e, axis=0, keepdims=True))).astype(BF)
                    pt_ref[slot + n, place * TOK : (place + 1) * TOK, lanes((p, p + 1))] = pt
    for n in range(count):
        vals = head_columns(kv[n * TOK : (n + 1) * TOK, TOK:])
        tokens = pl.ds(pl.multiple_of((slot + n) * TOK, TOK), TOK)
        for span, part in zip(GROUPS, vals):
            out = mm(part, pt_ref[slot + n, :, lanes(span)]).astype(BF)
            for p in range(*span):
                at_ref[lanes((p, p + 1)), tokens] = out[:, lanes((p - span[0], p - span[0] + 1))]
    return xf


def backward_clients(slot, count, cg_ref, wo_ref, q_ref, kv_ref, pt_ref, dq_ref, dkv_ref, datt_ref, ds_ref):
    size = count * TOK
    datt = mm(cg_ref[pl.ds(slot, count)].reshape(size, D), wo_ref[...], NT).astype(BF)
    for n in range(count):
        for p in range(PAIRS):
            datt_ref[n, p] = datt[n * TOK : (n + 1) * TOK, lanes((p, p + 1))]
    for place in range(2):
        keys_at = slice(place * TOK, (place + 1) * TOK)
        for head in range(2):
            span = MEETS[place][head]
            for n in range(count):
                vals = head_rows(kv_ref[slot + n, :, TOK:])
                d_probs = mm(vals[place][head], stack(datt_ref, n, span), NT)
                for p in range(*span):
                    wide = pt_ref[slot + n, keys_at, lanes((p, p + 1))].astype(F32)
                    both = d_probs[:, lanes((p - span[0], p - span[0] + 1))] * wide
                    ds = (both - wide * jnp.sum(both, axis=0, keepdims=True)) * SCALE
                    ds_ref[n, keys_at, lanes((p, p + 1))] = ds.astype(BF)
    low = lax.broadcasted_iota(jnp.int32, (TOK, TOK), 1) < HEAD_DIM
    for n in range(count):
        keys = head_columns(kv_ref[slot + n, :, :TOK])
        for span, part in zip(GROUPS, keys):
            out = mm(part, ds_ref[n, :, lanes(span)]).astype(BF)
            for p in range(*span):
                dq_ref[slot + n, :, lanes((p, p + 1))] = out[:, lanes((p - span[0], p - span[0] + 1))].T
        for at in range(2):
            left = (lambda k, l: ds_ref[n, k, l]) if at == 0 else (lambda k, l: pt_ref[slot + n, k, l])
            right = (lambda span: stack(q_ref, slot + n, span)) if at == 0 else (lambda span: stack(datt_ref, n, span))
            total = [
                [mm(left(slice(o * TOK, (o + 1) * TOK), lanes(span)), right(span)) for span in MEETS[o]] for o in range(2)
            ]
            first = total[0][0] + pltpu.roll(total[1][0], HEAD_DIM, 1)
            second = total[1][1] + pltpu.roll(total[0][1], HEAD_DIM, 1)
            dkv_ref[slot + n, :, lanes((at, at + 1))] = jnp.where(low, first, second).astype(BF)


def last_products(left_ref, pairs):
    step = D // 2

    @pl.loop(0, 2)
    def _(t):
        rows = pl.ds(pl.multiple_of(t * step, step), step)
        for right_ref, out_ref in pairs:
            right = right_ref[...].reshape(16 * TOK, right_ref.shape[-1])
            out_ref[rows, :] = (mm(left_ref[rows, :], right) * (1.0 / 16)).astype(BF)


def server_rows(j, mc_ref, sgain, ws_ref, served_ref, ns_ref, act_ref, sum_ref):
    size = 2 * TOK
    units = ws_ref.shape[1]
    hf = mc_ref[pl.ds(2 * j, 2)].reshape(size, D).astype(F32)
    cot = mc_ref[pl.ds(8 + 2 * j, 2)].reshape(size, D)
    inv = lax.rsqrt(jnp.mean(hf * hf, axis=-1, keepdims=True) + EPS)
    normed = (hf * inv * sgain).astype(BF)
    columns = pl.ds(pl.multiple_of(j * size, size), size)
    ns_ref[columns, :] = normed
    gate, up = mm(ws_ref[0], normed, NT), mm(ws_ref[1], normed, NT)
    d_hidden = mm(ws_ref[2], cot, NT)
    sigma = jax.nn.sigmoid(gate)
    silu = gate * sigma
    act_ref[2, :, columns] = (silu * up).astype(BF)
    act_ref[0, :, columns] = (d_hidden * up * sigma * (1.0 + gate * (1.0 - sigma))).astype(BF)
    act_ref[1, :, columns] = (d_hidden * silu).astype(BF)
    served = mm(act_ref[2, :, columns], ws_ref[2], TN).astype(BF)
    served_ref[pl.ds(2 * j, 2)] = served.reshape(2, TOK, D)
    both = act_ref[pl.ds(0, 2), :, columns].reshape(2 * units, size)
    scaled = mm(both, ws_ref[pl.ds(0, 2)].reshape(2 * units, D), TN) * sgain
    hf = mc_ref[pl.ds(2 * j, 2)].reshape(size, D).astype(F32)
    pushed = inv * scaled - hf * (inv * inv * inv) * jnp.mean(scaled * hf, axis=-1, keepdims=True)
    sum_ref[...] += pushed[:TOK] + pushed[TOK:]


def server_gradients(mc_ref, gr_ref, ns_ref, act_ref):
    width = gr_ref.shape[1] // 2

    @pl.loop(0, 2)
    def _(t):
        rows = pl.ds(pl.multiple_of(t * width, 16), width)
        gr_ref[0, rows, :] = mm(act_ref[0, rows, :], ns_ref[...]).astype(BF)
        gr_ref[1, rows, :] = mm(act_ref[1, rows, :], ns_ref[...]).astype(BF)
        gr_ref[2, rows, :] = mm(act_ref[2, rows, :], mc_ref[pl.ds(8, 8)].reshape(8 * TOK, D)).astype(BF)


def step_kernel(
    valid_ref, x_ref, cot_ref, gain_ref, sgain_ref, wq_hbm, wkv_hbm, wo_hbm, wg_hbm, wu_hbm, wd_hbm,
    out_ref, gq_hbm, gkv_hbm, go_hbm, own_g, own_u, own_d, got_g, got_u, got_d,
    wq_ref, wkv_ref, wo_ref, ws_ref, xs_ref, mc_ref, nt_ref, at_ref, q_ref, kv_ref, pt_ref, datt_ref, ds_ref,
    served_ref, gr_ref, ns_ref, act_ref, sum_ref, ls_ref, part_ref, mine_ref, slices_ref, cg_ref, back_ref, dkv_ref,
    load, send_m, recv_m, send_x, recv_x, send_w, recv_w, send_r, recv_r, send_a, recv_a,
    send_z, recv_z, send_c, recv_c, send_s, recv_s, send_g, recv_g, keep,
):
    pos = places()
    m, c = pos["m"], pos["c"]
    width = wg_hbm.shape[0]
    near, far = pl.ds(0, width), pl.ds(width, width)
    weights = (wg_hbm, wu_hbm, wd_hbm)
    loads = [
        pltpu.make_async_copy(s, d, load.at[k])
        for k, (s, d) in enumerate(
            [(wq_hbm, wq_ref), (wkv_hbm, wkv_ref), (wo_hbm, wo_ref)]
            + [(w, ws_ref.at[k, near]) for k, w in enumerate(weights)]
        )
    ]
    for copy in loads:
        copy.start()
    live = lax.broadcasted_iota(jnp.int32, (TOK, D), 0) < valid_ref[0, 0]
    mc_ref[8] = jnp.where(live, cot_ref[...].astype(F32), 0.0).astype(BF)
    xs_ref[0] = x_ref[...]

    peers = [{"mem": (m + d) % 16} for d in range(1, 16)]
    entry_barrier(peers + [pos[k] for k in ("zp", "zm", "lp")])
    lo, hi = pl.ds(0, HALF), pl.ds(HALF, HALF)

    def mem_copies(sems, base):
        at = lambda k: mc_ref.at[base + k]
        plan = [
            (at(0), at(1), "xp"),
            (at(0), at(2), "xm"),
            (at(0), at(3), "yp"),
            (mc_ref.at[base + 1, lo], mc_ref.at[base + 6, lo], "xp"),
            (mc_ref.at[base + 2, hi], mc_ref.at[base + 6, hi], "xm"),
            (at(3), at(4), "xp"),
            (at(3), at(5), "xm"),
            (at(6), at(7), "yp"),
        ]
        return [remote(s, d, send_m, recv_m, sems + k, pos[n]) for k, (s, d, n) in enumerate(plan)]

    cot, cut = mem_copies(0, 8), mem_copies(8, 0)

    def ring_copies(first, block, send, recv):
        ring = {}
        for stream in range(2):
            for way, name in ((0, "zp"), (1, "zm")):
                for step in range(1, 5):
                    before = stream if step == 1 else ring_slot(step - 1, stream, way)
                    after = ring_slot(step, stream, way)
                    src = first if before == 0 else block(before, step == 4, way)
                    k = 1 + (step - 1) * 4 + stream * 2 + way
                    ring[step, stream, way] = remote(src, block(after, step == 4, way), send, recv, k, pos[name])
        return remote(first, block(1, False, 0), send, recv, 0, pos["lp"]), ring

    def input_block(slot, halved, way):
        return xs_ref.at[slot, (lo, hi)[way]] if halved else xs_ref.at[slot]

    in_across, in_ring = ring_copies(x_ref, input_block, send_x, recv_x)
    swap = [remote(w, ws_ref.at[k, far], send_w, recv_w, k, pos["co"]) for k, w in enumerate(weights)]

    def grad_block(slot, halved, way):
        start, size = (way * 32, 32) if halved else (0, HALF)
        return cg_ref.at[slot, pl.ds(pl.multiple_of(c * HALF + start, 32), size)]

    cg_across, cg_ring = ring_copies(grad_block(0, False, 0), grad_block, send_z, recv_z)
    over = {
        slot: remote(grad_block(slot, False, 0), grad_block(slot, False, 0), send_c, recv_c, slot - 1, pos["co"])
        for slot in range(1, 16)
    }
    shares = [remote(ls_ref.at[(m + d) % 16], part_ref.at[d - 1], send_r, recv_r, d - 1, peers[d - 1]) for d in range(1, 16)]
    spread = [remote(mine_ref, slices_ref.at[m], send_a, recv_a, d, peers[d]) for d in range(15)]
    names = ("xm", "xp", "yp", "yxm", "yxp", "x2", "yx2")
    serve = [remote(served_ref.at[k + 1], back_ref.at[k], send_s, recv_s, k, pos[n]) for k, n in enumerate(names)]
    trade = [
        remote(gr_ref.at[k, far], got, send_g, recv_g, k, pos["co"]) for k, got in enumerate((got_g, got_u, got_d))
    ]
    keeps = [pltpu.make_async_copy(gr_ref.at[k, near], own, keep.at[k]) for k, own in enumerate((own_g, own_u, own_d))]

    for copy in [in_ring[1, 0, 0], in_ring[1, 0, 1]] + cot[:2] + [in_across, cot[2]] + swap:
        copy.start()
    sum_ref[...] = mc_ref[8].astype(F32)
    gain, sgain = gain_ref[...], sgain_ref[...]
    for copy in loads[:3]:
        copy.wait()
    saved = (nt_ref, at_ref, q_ref, kv_ref, pt_ref)
    xf = forward_clients(0, 1, xs_ref, gain, wq_ref, wkv_ref, *saved)
    mc_ref[0] = (xf + mm(at_ref[:, :TOK], wo_ref[...], TN)).astype(BF)
    for copy in cut[:3]:
        copy.start()

    def from_neighbours(copies):
        copies[0].wait_recv()
        copies[3].start()
        copies[1].wait_recv()
        copies[4].start()

    def from_across(copies):
        copies[2].wait_recv()
        copies[5].start()
        copies[6].start()

    def from_far(copies):
        copies[3].wait_recv()
        copies[4].wait_recv()
        copies[7].start()

    def inputs(step, stream):
        for way in range(2):
            in_ring[step, stream, way].wait_recv()
            if step < 4:
                in_ring[step + 1, stream, way].start()

    def first_inputs():
        in_across.wait_recv()
        in_ring[1, 1, 0].start()
        in_ring[1, 1, 1].start()

    def server_weights():
        for copy in loads[3:]:
            copy.wait()
        for copy in swap:
            copy.wait_recv()

    def arrived(*which):
        for copies in (cot, cut):
            for k in which:
                copies[k].wait_recv()

    def share():
        ls_ref[...] = sum_ref[...].reshape(16, 8, D).astype(BF)
        for copy in shares:
            copy.start()

    def gradients():
        server_gradients(mc_ref, gr_ref, ns_ref, act_ref)
        sum_ref[...] = mc_ref[0].astype(F32)

    def reduce():
        total = ls_ref[m].astype(F32)
        for d in range(15):
            shares[d].wait_recv()
            total = total + part_ref[d].astype(F32)
        mine_ref[...] = (total * (1.0 / 16)).astype(BF)
        for copy in spread:
            copy.start()
        slices_ref[m] = mine_ref[...]

    def own_group():
        for d in range(15):
            spread[d].wait_recv()
        cg_ref[0] = slices_ref[...].astype(F32).reshape(TOK, D).astype(BF)
        for copy in [cg_across, cg_ring[1, 0, 0], cg_ring[1, 0, 1]] + serve + trade + keeps:
            copy.start()

    def when_at(i, events):
        for at, todo in events.items():
            @pl.when(i == at)
            def _():
                for act in todo:
                    act()

    before_rows = {
        0: [lambda: from_neighbours(cot), lambda: inputs(1, 0), first_inputs],
        1: [server_weights, lambda: from_across(cot), lambda: from_neighbours(cut)],
        2: [lambda: from_across(cut), lambda: from_far(cot)],
        4: [lambda: inputs(3, 0), lambda: arrived(5, 6)],
        5: [lambda: arrived(7)],
        6: [lambda: inputs(3, 1), own_group],
        7: [lambda: inputs(4, 0), lambda: inputs(4, 1)],
    }
    before_pair = {
        1: [lambda: inputs(2, 0)],
        2: [lambda: inputs(1, 1), lambda: from_far(cut)],
        4: [lambda: inputs(2, 1)],
        5: [share, gradients, reduce],
    }
    order = sum(pair << (3 * k) for k, pair in enumerate((1, 3, 0, 2, 5, 4, 6, 7)))

    @pl.loop(0, 8)
    def _(k):
        when_at(k, before_rows)

        @pl.when((k % 3 != 0) & (k < 6))
        def _():
            server_rows(k - 1 - k // 4, mc_ref, sgain, ws_ref, served_ref, ns_ref, act_ref, sum_ref)

        when_at(k, before_pair)
        pair = jnp.right_shift(order, 3 * k) % 8
        forward_clients(2 * pair, 2, xs_ref, gain, wq_ref, wkv_ref, *saved)

    def grads(step, stream):
        for way in range(2):
            cg_ring[step, stream, way].wait_recv()
            if step < 4:
                cg_ring[step + 1, stream, way].start()
                over[ring_slot(step, stream, way)].start()
        if step == 4:
            over[14 + stream].start()

    def first_grads():
        cg_across.wait_recv()
        cg_ring[1, 1, 0].start()
        cg_ring[1, 1, 1].start()
        over[1].start()

    def handed(*slots):
        for slot in slots:
            over[slot].wait_recv()

    for copy in cot + cut:
        copy.wait_send()
    backward_events = {
        0: [first_grads, lambda: grads(1, 0), lambda: handed(1)],
        1: [lambda: grads(1, 1), lambda: handed(2, 3)],
        2: [lambda: grads(2, 0), lambda: handed(4, 5)],
        3: [lambda: grads(2, 1), lambda: handed(6, 7)],
        4: [lambda: grads(3, 0), lambda: handed(8, 9)],
        5: [lambda: grads(3, 1), lambda: handed(10, 11)],
        6: [lambda: grads(4, 0), lambda: grads(4, 1), lambda: handed(12, 13)],
        7: [lambda: handed(14, 15)],
    }

    @pl.loop(0, 8)
    def _(j):
        when_at(j, backward_events)
        backward_clients(2 * j, 2, cg_ref, wo_ref, q_ref, kv_ref, pt_ref, mc_ref, dkv_ref, datt_ref, ds_ref)

    go_ref = ns_ref.at[pl.ds(0, D)]
    done = [
        pltpu.make_async_copy(s, d, load.at[k])
        for k, (s, d) in enumerate([(go_ref, go_hbm), (wq_ref, gq_hbm), (wkv_ref, gkv_hbm)])
    ]
    last_products(at_ref, [(cg_ref, go_ref)])
    done[0].start()
    last_products(nt_ref, [(mc_ref, wq_ref), (dkv_ref, wkv_ref)])
    done[1].start()
    done[2].start()

    for copy in serve:
        copy.wait_recv()
    out = sum_ref[...] + served_ref[0].astype(F32)
    for k in range(7):
        out = out + back_ref[k].astype(F32)
    out_ref[...] = out.astype(BF)
    for copy in trade:
        copy.wait_recv()
    for copy in keeps + done:
        copy.wait()
    for copy in [in_across, cg_across] + list(in_ring.values()) + list(cg_ring.values()) + list(over.values()):
        copy.wait_send()
    for copy in swap + shares + spread + serve + trade:
        copy.wait_send()


def step_call(valid, x, cot, gain, sgain, wq, wkv, wo, wg, wu, wd):
    vmem, anyspace = pl.BlockSpec(memory_space=pltpu.VMEM), pl.BlockSpec(memory_space=pl.ANY)
    sds = jax.ShapeDtypeStruct
    sem = pltpu.SemaphoreType.DMA
    width = wg.shape[0]
    units = 2 * width
    block = pltpu.VMEM((TOK, D), BF)
    blocks = lambda n: pltpu.VMEM((n, TOK, D), BF)
    return pl.pallas_call(
        step_kernel,
        out_shape=(
            sds((TOK, D), BF), sds((D, D), BF), sds((D, 2 * TOK), BF), sds((D, D), BF),
            *[sds((width, D), BF)] * 6,
        ),
        in_specs=[pl.BlockSpec(memory_space=pltpu.SMEM)] + [vmem] * 4 + [anyspace] * 6,
        out_specs=[vmem] + [anyspace] * 9,
        scratch_shapes=[
            pltpu.VMEM((D, D), BF), pltpu.VMEM((D, 2 * TOK), BF), pltpu.VMEM((D, D), BF), pltpu.VMEM((3, units, D), BF),
            blocks(16), blocks(16), pltpu.VMEM((D, 16 * TOK), BF), pltpu.VMEM((D, 16 * TOK), BF),
            pltpu.VMEM((16, PAIRS, TOK, TOK), BF), pltpu.VMEM((16, TOK, 2 * TOK), BF), pltpu.VMEM((16, 2 * TOK, D), BF),
            pltpu.VMEM((2, PAIRS, TOK, TOK), BF), pltpu.VMEM((2, 2 * TOK, D), BF),
            blocks(8), pltpu.VMEM((3, units, D), BF), pltpu.VMEM((8 * TOK, D), BF), pltpu.VMEM((3, units, 8 * TOK), BF),
            pltpu.VMEM((TOK, D), F32), pltpu.VMEM((16, 8, D), BF), pltpu.VMEM((15, 8, D), BF), pltpu.VMEM((8, D), BF),
            pltpu.VMEM((16, 8, D), BF), blocks(16), blocks(7), pltpu.VMEM((16, TOK, 2 * TOK), BF),
            sem((6,)), sem((16,)), sem((16,)), sem((17,)), sem((17,)), sem((3,)), sem((3,)), sem((15,)), sem((15,)),
            sem((15,)), sem((15,)), sem((17,)), sem((17,)), sem((15,)), sem((15,)), sem((7,)), sem((7,)),
            sem((3,)), sem((3,)), sem((3,)),
        ],
        compiler_params=pltpu.CompilerParams(collective_id=0, has_side_effects=True, vmem_limit_bytes=60 * 1024 * 2**10),
        name="split_step",
    )(valid, x, cot, gain, sgain, wq, wkv, wo, wg, wu, wd)


def on_device(
    client_input, client_gain, w_query, w_keyval, w_out, server_gain, w_gate, w_up, w_down, out_grad, valid
):
    server_out, grad_q, grad_kv, grad_o, *shards = step_call(
        valid, client_input[0, 0], out_grad[0, 0], client_gain, server_gain, w_query[0], w_keyval[0], w_out[0],
        w_gate[0].T, w_up[0].T, w_down[0],
    )
    gate, up, down = [(own.astype(F32) + got.astype(F32)).astype(BF) for own, got in zip(shards[:3], shards[3:])]
    return (
        server_out[None, None],
        grad_q[None],
        grad_kv[None],
        grad_o[None],
        gate.T[None],
        up.T[None],
        down[None],
    )


def solution(mesh):
    in_specs = (
        P("grp", "mem", None, None),
        P("mem", None),
        P("mem", None, None),
        P("mem", None, None),
        P("mem", None, None),
        P("grp", None),
        P("grp", None, "mem"),
        P("grp", None, "mem"),
        P("grp", "mem", None),
        P("grp", "mem", None, None),
        P("grp", "mem"),
    )
    out_specs = (
        P("grp", "mem", None, None),
        P("mem", None, None),
        P("mem", None, None),
        P("mem", None, None),
        P("grp", None, "mem"),
        P("grp", None, "mem"),
        P("grp", "mem", None),
    )
    return jax.shard_map(
        on_device, mesh=mesh, in_specs=in_specs, out_specs=out_specs, check_vma=False
    )
```

```python
import functools

import jax
import jax.numpy as jnp
from jax import lax
from jax.experimental import pallas as pl
from jax.experimental.pallas import tpu as pltpu
from jax.sharding import PartitionSpec as P

EPS = 1e-06
HEAD_DIM = 64
TOK = 128
D = 896
PAIRS = 7
BF = jnp.bfloat16
F32 = jnp.float32
MESH = pl.DeviceIdType.MESH
NN = (((1,), (0,)), ((), ()))
NT = (((1,), (1,)), ((), ()))
TN = (((0,), (0,)), ((), ()))
HALF = TOK // 2
SCALE = HEAD_DIM ** (-0.5)


def mm(a, b, dims=NN):
    return lax.dot_general(a, b, dims, preferred_element_type=F32)


def places():
    g, m = lax.axis_index("grp"), lax.axis_index("mem")
    l, z = g // 8, g % 8
    yh, x, c = m // 8, (m // 2) % 4, m % 2
    at = lambda y_, x_, c_: {"mem": y_ * 8 + x_ * 2 + c_}
    return dict(
        m=m,
        c=c,
        xp=at(yh, (x + 1) % 4, c),
        xm=at(yh, (x + 3) % 4, c),
        x2=at(yh, (x + 2) % 4, c),
        yp=at(1 - yh, x, c),
        yxp=at(1 - yh, (x + 1) % 4, c),
        yxm=at(1 - yh, (x + 3) % 4, c),
        yx2=at(1 - yh, (x + 2) % 4, c),
        co=at(yh, x, 1 - c),
        zp={"grp": l * 8 + (z + 1) % 8},
        zm={"grp": l * 8 + (z + 7) % 8},
        lp={"grp": (1 - l) * 8 + z},
    )


def remote(src, dst, send, recv, k, device):
    return pltpu.make_async_remote_copy(
        src_ref=src, dst_ref=dst, send_sem=send.at[k], recv_sem=recv.at[k], device_id=device, device_id_type=MESH
    )


def entry_barrier(devices):
    barrier = pltpu.get_barrier_semaphore()
    for device in devices:
        pl.semaphore_signal(barrier, inc=1, device_id=device, device_id_type=MESH)
    pl.semaphore_wait(barrier, len(devices))


def ring_slot(step, stream, way):
    return 2 + 4 * (step - 1) + 2 * stream + way if step < 4 else 14 + stream


MEETS = (((0, 4), (4, 7)), ((0, 3), (3, 7)))
GROUPS = ((0, 3), (3, 4), (4, 7))


def head_rows(both, scale=1.0):
    wide = both.astype(F32) * scale
    turned = pltpu.roll(wide, HEAD_DIM, 1)
    low = lax.broadcasted_iota(jnp.int32, wide.shape, 1) < HEAD_DIM
    zero = jnp.zeros_like(wide)
    first = (jnp.where(low, wide, zero).astype(BF), jnp.where(low, turned, zero).astype(BF))
    second = (jnp.where(low, zero, turned).astype(BF), jnp.where(low, zero, wide).astype(BF))
    return first, second


def head_columns(both):
    turned = both.T
    zero = jnp.zeros((HEAD_DIM, TOK), BF)
    heads = (turned[:HEAD_DIM], turned[HEAD_DIM:])
    build = lambda a, b: jnp.concatenate(
        [jnp.concatenate([heads[a], zero], axis=1), jnp.concatenate([zero, heads[b]], axis=1)], axis=0
    )
    return build(0, 0), build(0, 1), build(1, 1)


def lanes(span):
    return slice(span[0] * TOK, span[1] * TOK)


def stack(ref, n, span):
    return ref[n, span[0] : span[1]].reshape((span[1] - span[0]) * TOK, TOK)


def forward_clients(slot, count, xs_ref, gain, wq_ref, wkv_ref, nt_ref, at_ref, q_ref, kv_ref, pt_ref):
    size = count * TOK
    xf = xs_ref[pl.ds(slot, count)].reshape(size, D).astype(F32)
    inv = lax.rsqrt(jnp.mean(xf * xf, axis=-1, keepdims=True) + EPS)
    normed = (xf * inv * gain).astype(BF)
    columns = pl.ds(pl.multiple_of(slot * TOK, TOK), size)
    nt_ref[:, columns] = normed.T
    queries = mm(normed, wq_ref[...]).astype(BF)
    kv = mm(normed, wkv_ref[...]).astype(BF)
    kv_ref[pl.ds(slot, count)] = kv.reshape(count, TOK, 2 * TOK)
    for n in range(count):
        for p in range(PAIRS):
            q_ref[slot + n, p] = queries[n * TOK : (n + 1) * TOK, lanes((p, p + 1))]
    s_at = lax.broadcasted_iota(jnp.int32, (TOK, TOK), 0)
    t_at = lax.broadcasted_iota(jnp.int32, (TOK, TOK), 1)
    seen = s_at <= t_at
    for place in range(2):
        for head in range(2):
            span = MEETS[place][head]
            for n in range(count):
                keys = head_rows(kv[n * TOK : (n + 1) * TOK, :TOK], SCALE)
                scores = mm(keys[place][head], stack(q_ref, slot + n, span), NT)
                for p in range(*span):
                    s = jnp.where(seen, scores[:, lanes((p - span[0], p - span[0] + 1))], -1e30)
                    e = jnp.exp(s - jnp.max(s, axis=0, keepdims=True))
                    pt = (e * (1.0 / jnp.sum(e, axis=0, keepdims=True))).astype(BF)
                    pt_ref[slot + n, place * TOK : (place + 1) * TOK, lanes((p, p + 1))] = pt
    for n in range(count):
        vals = head_columns(kv[n * TOK : (n + 1) * TOK, TOK:])
        tokens = pl.ds(pl.multiple_of((slot + n) * TOK, TOK), TOK)
        for span, part in zip(GROUPS, vals):
            out = mm(part, pt_ref[slot + n, :, lanes(span)]).astype(BF)
            for p in range(*span):
                at_ref[lanes((p, p + 1)), tokens] = out[:, lanes((p - span[0], p - span[0] + 1))]
    return xf


def backward_clients(slot, count, cg_ref, wo_ref, q_ref, kv_ref, pt_ref, dq_ref, dkv_ref, datt_ref, ds_ref):
    size = count * TOK
    datt = mm(cg_ref[pl.ds(slot, count)].reshape(size, D), wo_ref[...], NT).astype(BF)
    for n in range(count):
        for p in range(PAIRS):
            datt_ref[n, p] = datt[n * TOK : (n + 1) * TOK, lanes((p, p + 1))]
    for place in range(2):
        keys_at = slice(place * TOK, (place + 1) * TOK)
        for head in range(2):
            span = MEETS[place][head]
            for n in range(count):
                vals = head_rows(kv_ref[slot + n, :, TOK:])
                d_probs = mm(vals[place][head], stack(datt_ref, n, span), NT)
                for p in range(*span):
                    wide = pt_ref[slot + n, keys_at, lanes((p, p + 1))].astype(F32)
                    both = d_probs[:, lanes((p - span[0], p - span[0] + 1))] * wide
                    ds = both - wide * jnp.sum(both, axis=0, keepdims=True)
                    ds_ref[n, keys_at, lanes((p, p + 1))] = ds.astype(BF)
    low = lax.broadcasted_iota(jnp.int32, (TOK, TOK), 1) < HEAD_DIM
    for n in range(count):
        keys = head_columns((kv_ref[slot + n, :, :TOK].astype(F32) * SCALE).astype(BF))
        for span, part in zip(GROUPS, keys):
            out = mm(part, ds_ref[n, :, lanes(span)]).astype(BF)
            for p in range(*span):
                dq_ref[slot + n, :, lanes((p, p + 1))] = out[:, lanes((p - span[0], p - span[0] + 1))].T
        for at in range(2):
            left = (lambda k, l: ds_ref[n, k, l]) if at == 0 else (lambda k, l: pt_ref[slot + n, k, l])
            right = (lambda span: stack(q_ref, slot + n, span)) if at == 0 else (lambda span: stack(datt_ref, n, span))
            total = [
                [mm(left(slice(o * TOK, (o + 1) * TOK), lanes(span)), right(span)) for span in MEETS[o]] for o in range(2)
            ]
            first = total[0][0] + pltpu.roll(total[1][0], HEAD_DIM, 1)
            second = total[1][1] + pltpu.roll(total[0][1], HEAD_DIM, 1)
            dkv_ref[slot + n, :, lanes((at, at + 1))] = (jnp.where(low, first, second) * (SCALE if at == 0 else 1.0)).astype(BF)


def last_products(left_ref, rows, pairs):
    for right_ref, out_ref in pairs:
        right = right_ref[...].reshape(16 * TOK, right_ref.shape[-1])
        out_ref[rows, :] = (mm(left_ref[rows, :], right) * (1.0 / 16)).astype(BF)


def finish_kernel(
    served_hbm, nt_hbm, at_hbm, dq_hbm, dkv_hbm, cg_hbm, own_g, own_u, own_d, got_g, got_u, got_d,
    out_hbm, gq_hbm, gkv_hbm, go_hbm, gate_hbm, up_hbm, down_hbm,
    served_ref, nt_ref, at_ref, dq_ref, dkv_ref, cg_ref, own_ref, got_ref, gq_ref, gkv_ref, go_ref, load, store,
):
    half = D // 2
    top, low = pl.ds(0, half), pl.ds(half, half)
    moves = [
        (cg_hbm, cg_ref), (at_hbm.at[top], at_ref.at[top]), (at_hbm.at[low], at_ref.at[low]),
        (own_g, own_ref.at[0]), (own_u, own_ref.at[1]), (own_d, own_ref.at[2]),
        (got_g, got_ref.at[0]), (got_u, got_ref.at[1]), (got_d, got_ref.at[2]),
        (served_hbm, served_ref), (dq_hbm, dq_ref), (dkv_hbm, dkv_ref),
        (nt_hbm.at[top], nt_ref.at[top]), (nt_hbm.at[low], nt_ref.at[low]),
    ]
    loads = [pltpu.make_async_copy(s, d, load.at[k]) for k, (s, d) in enumerate(moves)]
    for copy in loads:
        copy.start()
    stores = [
        (go_ref, go_hbm), (own_ref.at[0], gate_hbm), (own_ref.at[1], up_hbm), (own_ref.at[2], down_hbm),
        (served_ref, out_hbm), (gq_ref.at[top], gq_hbm.at[top]), (gkv_ref.at[top], gkv_hbm.at[top]),
        (gq_ref.at[low], gq_hbm.at[low]), (gkv_ref.at[low], gkv_hbm.at[low]),
    ]
    stores = [pltpu.make_async_copy(s, d, store.at[k]) for k, (s, d) in enumerate(stores)]

    def await_loads(*which):
        for k in which:
            loads[k].wait()

    @pl.loop(0, 2)
    def _(t):
        @pl.when(t == 0)
        def _():
            await_loads(0, 1)

        @pl.when(t == 1)
        def _():
            await_loads(2)

        last_products(at_ref, pl.ds(pl.multiple_of(t * half, 64), half), [(cg_ref, go_ref)])

    await_loads(*range(3, 10))
    stores[4].start()
    for k in range(3):
        own_ref[k] = (own_ref[k].astype(F32) + got_ref[k].astype(F32)).astype(BF)
    stores[0].start()

    @pl.loop(0, 2)
    def _(t):
        @pl.when(t == 0)
        def _():
            await_loads(10, 11, 12)
            for copy in stores[1:4]:
                copy.start()

        @pl.when(t == 1)
        def _():
            await_loads(13)
            for copy in stores[5:7]:
                copy.start()

        last_products(nt_ref, pl.ds(pl.multiple_of(t * half, 64), half), [(dq_ref, gq_ref), (dkv_ref, gkv_ref)])

    for copy in stores[7:]:
        copy.start()
    for copy in stores:
        copy.wait()


def finish_call(*args):
    anyspace = pl.BlockSpec(memory_space=pl.ANY)
    sds = jax.ShapeDtypeStruct
    width = args[6].shape[0]
    blocks = lambda n: pltpu.VMEM((n, TOK, D), BF)
    return pl.pallas_call(
        finish_kernel,
        out_shape=(
            sds((TOK, D), BF), sds((D, D), BF), sds((D, 2 * TOK), BF), sds((D, D), BF), *[sds((width, D), BF)] * 3,
        ),
        in_specs=[anyspace] * 12,
        out_specs=[anyspace] * 7,
        scratch_shapes=[
            pltpu.VMEM((TOK, D), BF), pltpu.VMEM((D, 16 * TOK), BF), pltpu.VMEM((D, 16 * TOK), BF), blocks(16),
            pltpu.VMEM((16, TOK, 2 * TOK), BF), blocks(16), pltpu.VMEM((3, width, D), BF), pltpu.VMEM((3, width, D), BF),
            pltpu.VMEM((D, D), BF), pltpu.VMEM((D, 2 * TOK), BF), pltpu.VMEM((D, D), BF),
            pltpu.SemaphoreType.DMA((14,)), pltpu.SemaphoreType.DMA((9,)),
        ],
        compiler_params=pltpu.CompilerParams(vmem_limit_bytes=60 * 1024 * 2**10),
        name="finish",
    )(*args)


def server_rows(j, mc_ref, sgain, ws_ref, served_ref, ns_ref, act_ref, sum_ref):
    size = 2 * TOK
    units = ws_ref.shape[1]
    hf = mc_ref[pl.ds(2 * j, 2)].reshape(size, D).astype(F32)
    cot = mc_ref[pl.ds(8 + 2 * j, 2)].reshape(size, D)
    inv = lax.rsqrt(jnp.mean(hf * hf, axis=-1, keepdims=True) + EPS)
    normed = (hf * inv * sgain).astype(BF)
    columns = pl.ds(pl.multiple_of(j * size, size), size)
    ns_ref[columns, :] = normed
    gate, up = mm(ws_ref[0], normed, NT), mm(ws_ref[1], normed, NT)
    d_hidden = mm(ws_ref[2], cot, NT)
    sigma = jax.nn.sigmoid(gate)
    silu = gate * sigma
    act_ref[2, :, columns] = (silu * up).astype(BF)
    act_ref[0, :, columns] = (d_hidden * up * sigma * (1.0 + gate * (1.0 - sigma))).astype(BF)
    act_ref[1, :, columns] = (d_hidden * silu).astype(BF)
    served = mm(act_ref[2, :, columns], ws_ref[2], TN).astype(BF)
    served_ref[pl.ds(2 * j, 2)] = served.reshape(2, TOK, D)
    both = act_ref[pl.ds(0, 2), :, columns].reshape(2 * units, size)
    scaled = mm(both, ws_ref[pl.ds(0, 2)].reshape(2 * units, D), TN) * sgain
    hf = mc_ref[pl.ds(2 * j, 2)].reshape(size, D).astype(F32)
    pushed = inv * scaled - hf * (inv * inv * inv) * jnp.mean(scaled * hf, axis=-1, keepdims=True)
    sum_ref[...] += pushed[:TOK] + pushed[TOK:]


def server_gradients(mc_ref, gr_ref, ns_ref, act_ref):
    width = gr_ref.shape[1] // 2

    @pl.loop(0, 2)
    def _(t):
        rows = pl.ds(pl.multiple_of(t * width, 16), width)
        gr_ref[0, rows, :] = mm(act_ref[0, rows, :], ns_ref[...]).astype(BF)
        gr_ref[1, rows, :] = mm(act_ref[1, rows, :], ns_ref[...]).astype(BF)
        gr_ref[2, rows, :] = mm(act_ref[2, rows, :], mc_ref[pl.ds(8, 8)].reshape(8 * TOK, D)).astype(BF)


def step_kernel(
    valid_ref, x_ref, cot_ref, gain_ref, sgain_ref, wq_hbm, wkv_hbm, wo_hbm, wg_hbm, wu_hbm, wd_hbm,
    out_ref, nt_hbm, at_hbm, dq_hbm, dkv_hbm, cg_hbm, own_g, own_u, own_d, got_g, got_u, got_d,
    wq_ref, wkv_ref, wo_ref, ws_ref, xs_ref, mc_ref, nt_ref, at_ref, q_ref, kv_ref, pt_ref, datt_ref, ds_ref,
    served_ref, gr_ref, ns_ref, act_ref, sum_ref, ls_ref, part_ref, mine_ref, slices_ref, cg_ref, back_ref, dkv_ref,
    load, send_m, recv_m, send_x, recv_x, send_w, recv_w, send_r, recv_r, send_a, recv_a,
    send_z, recv_z, send_c, recv_c, send_s, recv_s, send_g, recv_g, keep, leave_sem,
):
    pos = places()
    m, c = pos["m"], pos["c"]
    width = wg_hbm.shape[0]
    near, far = pl.ds(0, width), pl.ds(width, width)
    weights = (wg_hbm, wu_hbm, wd_hbm)
    loads = [
        pltpu.make_async_copy(s, d, load.at[k])
        for k, (s, d) in enumerate(
            [(wq_hbm, wq_ref), (wkv_hbm, wkv_ref), (wo_hbm, wo_ref)]
            + [(w, ws_ref.at[k, near]) for k, w in enumerate(weights)]
        )
    ]
    for copy in loads:
        copy.start()
    live = lax.broadcasted_iota(jnp.int32, (TOK, D), 0) < valid_ref[0, 0]
    mc_ref[8] = jnp.where(live, cot_ref[...].astype(F32), 0.0).astype(BF)
    xs_ref[0] = x_ref[...]

    peers = [{"mem": (m + d) % 16} for d in range(1, 16)]
    entry_barrier(peers + [pos[k] for k in ("zp", "zm", "lp")])
    lo, hi = pl.ds(0, HALF), pl.ds(HALF, HALF)

    def mem_copies(sems, base):
        at = lambda k: mc_ref.at[base + k]
        plan = [
            (at(0), at(1), "xp"),
            (at(0), at(2), "xm"),
            (at(0), at(3), "yp"),
            (mc_ref.at[base + 1, lo], mc_ref.at[base + 6, lo], "xp"),
            (mc_ref.at[base + 2, hi], mc_ref.at[base + 6, hi], "xm"),
            (at(3), at(4), "xp"),
            (at(3), at(5), "xm"),
            (at(6), at(7), "yp"),
        ]
        return [remote(s, d, send_m, recv_m, sems + k, pos[n]) for k, (s, d, n) in enumerate(plan)]

    cot, cut = mem_copies(0, 8), mem_copies(8, 0)

    def ring_copies(first, block, send, recv):
        ring = {}
        for stream in range(2):
            for way, name in ((0, "zp"), (1, "zm")):
                for step in range(1, 5):
                    before = stream if step == 1 else ring_slot(step - 1, stream, way)
                    after = ring_slot(step, stream, way)
                    src = first if before == 0 else block(before, step == 4, way)
                    k = 1 + (step - 1) * 4 + stream * 2 + way
                    ring[step, stream, way] = remote(src, block(after, step == 4, way), send, recv, k, pos[name])
        return remote(first, block(1, False, 0), send, recv, 0, pos["lp"]), ring

    def input_block(slot, halved, way):
        return xs_ref.at[slot, (lo, hi)[way]] if halved else xs_ref.at[slot]

    in_across, in_ring = ring_copies(x_ref, input_block, send_x, recv_x)
    swap = [remote(w, ws_ref.at[k, far], send_w, recv_w, k, pos["co"]) for k, w in enumerate(weights)]

    def grad_block(slot, halved, way):
        start, size = (way * 32, 32) if halved else (0, HALF)
        return cg_ref.at[slot, pl.ds(pl.multiple_of(c * HALF + start, 32), size)]

    cg_across, cg_ring = ring_copies(grad_block(0, False, 0), grad_block, send_z, recv_z)
    over = {
        slot: remote(grad_block(slot, False, 0), grad_block(slot, False, 0), send_c, recv_c, slot - 1, pos["co"])
        for slot in range(1, 16)
    }
    shares = [remote(ls_ref.at[(m + d) % 16], part_ref.at[d - 1], send_r, recv_r, d - 1, peers[d - 1]) for d in range(1, 16)]
    spread = [remote(mine_ref, slices_ref.at[m], send_a, recv_a, d, peers[d]) for d in range(15)]
    names = ("xm", "xp", "yp", "yxm", "yxp", "x2", "yx2")
    serve = [remote(served_ref.at[k + 1], back_ref.at[k], send_s, recv_s, k, pos[n]) for k, n in enumerate(names)]
    trade = [
        remote(gr_ref.at[k, far], got, send_g, recv_g, k, pos["co"]) for k, got in enumerate((got_g, got_u, got_d))
    ]
    keeps = [pltpu.make_async_copy(gr_ref.at[k, near], own, keep.at[k]) for k, own in enumerate((own_g, own_u, own_d))]

    for copy in [in_ring[1, 0, 0], in_ring[1, 0, 1]] + cot[:2] + [in_across, cot[2]]:
        copy.start()
    sum_ref[...] = mc_ref[8].astype(F32)
    gain, sgain = gain_ref[...], sgain_ref[...]
    for copy in loads[:3]:
        copy.wait()
    saved = (nt_ref, at_ref, q_ref, kv_ref, pt_ref)
    xf = forward_clients(0, 1, xs_ref, gain, wq_ref, wkv_ref, *saved)
    mc_ref[0] = (xf + mm(at_ref[:, :TOK], wo_ref[...], TN)).astype(BF)
    for copy in cut[:3] + swap:
        copy.start()

    def from_neighbours(copies):
        copies[0].wait_recv()
        copies[3].start()
        copies[1].wait_recv()
        copies[4].start()

    def from_across(copies):
        copies[2].wait_recv()
        copies[5].start()
        copies[6].start()

    def from_far(copies):
        copies[3].wait_recv()
        copies[4].wait_recv()
        copies[7].start()

    def inputs(step, stream):
        for way in range(2):
            in_ring[step, stream, way].wait_recv()
            if step < 4:
                in_ring[step + 1, stream, way].start()

    def first_inputs():
        in_across.wait_recv()
        in_ring[1, 1, 0].start()
        in_ring[1, 1, 1].start()

    def server_weights():
        for copy in loads[3:]:
            copy.wait()
        for copy in swap:
            copy.wait_recv()

    def arrived(*which):
        for copies in (cot, cut):
            for k in which:
                copies[k].wait_recv()

    def share():
        ls_ref[...] = sum_ref[...].reshape(16, 8, D).astype(BF)
        for copy in shares:
            copy.start()

    def gradients():
        server_gradients(mc_ref, gr_ref, ns_ref, act_ref)
        sum_ref[...] = mc_ref[0].astype(F32)

    def reduce():
        total = ls_ref[m].astype(F32)
        for d in range(15):
            shares[d].wait_recv()
            total = total + part_ref[d].astype(F32)
        mine_ref[...] = (total * (1.0 / 16)).astype(BF)
        for copy in spread:
            copy.start()
        slices_ref[m] = mine_ref[...]

    def own_group():
        for d in range(15):
            spread[d].wait_recv()
        cg_ref[0] = slices_ref[...].astype(F32).reshape(TOK, D).astype(BF)
        for copy in [cg_across, cg_ring[1, 0, 0], cg_ring[1, 0, 1]] + trade + keeps:
            copy.start()

    def when_at(i, events):
        for at, todo in events.items():
            @pl.when(i == at)
            def _():
                for act in todo:
                    act()

    def go(copies):
        for copy in copies:
            copy.start()

    before_rows = {
        0: [lambda: from_neighbours(cot), lambda: inputs(1, 0), first_inputs],
        1: [server_weights, lambda: from_across(cot), lambda: from_neighbours(cut)],
        2: [lambda: from_across(cut), lambda: from_far(cot)],
        3: [lambda: arrived(5, 6)],
        4: [lambda: arrived(7)],
        5: [gradients, reduce],
        6: [lambda: inputs(3, 1)],
        7: [lambda: inputs(4, 0), lambda: inputs(4, 1), own_group],
    }
    before_pair = {
        1: [lambda: inputs(2, 0)],
        2: [lambda: inputs(1, 1), lambda: from_far(cut)],
        3: [lambda: go(serve[:3])],
        4: [share, lambda: inputs(3, 0), lambda: inputs(2, 1)],
    }
    order = sum(pair << (3 * k) for k, pair in enumerate((1, 3, 0, 2, 5, 4, 6, 7)))

    @pl.loop(0, 8)
    def _(k):
        when_at(k, before_rows)

        @pl.when((k >= 1) & (k <= 4))
        def _():
            server_rows(k - 1, mc_ref, sgain, ws_ref, served_ref, ns_ref, act_ref, sum_ref)

        when_at(k, before_pair)
        pair = jnp.right_shift(order, 3 * k) % 8
        forward_clients(2 * pair, 2, xs_ref, gain, wq_ref, wkv_ref, *saved)

    def grads(step, stream):
        for way in range(2):
            cg_ring[step, stream, way].wait_recv()
            if step < 4:
                cg_ring[step + 1, stream, way].start()
                over[ring_slot(step, stream, way)].start()
        if step == 4:
            over[14 + stream].start()

    def first_grads():
        cg_across.wait_recv()
        cg_ring[1, 1, 0].start()
        cg_ring[1, 1, 1].start()
        over[1].start()

    def handed(*slots):
        for slot in slots:
            over[slot].wait_recv()

    for copy in cot + cut:
        copy.wait_send()
    whole = pltpu.make_async_copy(cg_ref, cg_hbm, load.at[0])
    strip = D // 8
    leave = [
        [
            pltpu.make_async_copy(s.at[pl.ds(size * j, size)], d.at[pl.ds(size * j, size)], leave_sem.at[4 * j + k])
            for k, (s, d, size) in enumerate(
                [(nt_ref, nt_hbm, strip), (at_ref, at_hbm, strip), (mc_ref, dq_hbm, 2), (dkv_ref, dkv_hbm, 2)]
            )
        ]
        for j in range(8)
    ]

    backward_events = {
        0: [first_grads, lambda: grads(1, 0), lambda: handed(1)],
        1: [lambda: grads(1, 1), lambda: handed(2, 3), lambda: go(serve[3:] + leave[0])],
        2: [lambda: grads(2, 0), lambda: handed(4, 5), lambda: go(leave[1])],
        3: [lambda: grads(2, 1), lambda: handed(6, 7), lambda: go(leave[2])],
        4: [lambda: grads(3, 0), lambda: handed(8, 9), lambda: go(leave[3])],
        5: [lambda: grads(3, 1), lambda: handed(10, 11), lambda: go(leave[4])],
        6: [lambda: grads(4, 0), lambda: grads(4, 1), lambda: handed(12, 13), lambda: go(leave[5] + leave[7][:2])],
        7: [lambda: handed(14, 15), lambda: go(leave[6] + [whole])],
    }

    @pl.loop(0, 8)
    def _(j):
        when_at(j, backward_events)
        backward_clients(2 * j, 2, cg_ref, wo_ref, q_ref, kv_ref, pt_ref, mc_ref, dkv_ref, datt_ref, ds_ref)

    for copy in leave[7][2:]:
        copy.start()
    for copy in serve:
        copy.wait_recv()
    out = sum_ref[...] + served_ref[0].astype(F32)
    for k in range(7):
        out = out + back_ref[k].astype(F32)
    out_ref[...] = out.astype(BF)
    for copy in trade:
        copy.wait_recv()
    for copy in keeps + [whole] + sum(leave, []):
        copy.wait()
    for copy in [in_across, cg_across] + list(in_ring.values()) + list(cg_ring.values()) + list(over.values()):
        copy.wait_send()
    for copy in swap + shares + spread + serve + trade:
        copy.wait_send()


def step_call(valid, x, cot, gain, sgain, wq, wkv, wo, wg, wu, wd):
    vmem, anyspace = pl.BlockSpec(memory_space=pltpu.VMEM), pl.BlockSpec(memory_space=pl.ANY)
    sds = jax.ShapeDtypeStruct
    sem = pltpu.SemaphoreType.DMA
    width = wg.shape[0]
    units = 2 * width
    block = pltpu.VMEM((TOK, D), BF)
    blocks = lambda n: pltpu.VMEM((n, TOK, D), BF)
    return pl.pallas_call(
        step_kernel,
        out_shape=(
            sds((TOK, D), BF), sds((D, 16 * TOK), BF), sds((D, 16 * TOK), BF), sds((16, TOK, D), BF),
            sds((16, TOK, 2 * TOK), BF), sds((16, TOK, D), BF), *[sds((width, D), BF)] * 6,
        ),
        in_specs=[pl.BlockSpec(memory_space=pltpu.SMEM)] + [vmem] * 4 + [anyspace] * 6,
        out_specs=[vmem] + [anyspace] * 11,
        scratch_shapes=[
            pltpu.VMEM((D, D), BF), pltpu.VMEM((D, 2 * TOK), BF), pltpu.VMEM((D, D), BF), pltpu.VMEM((3, units, D), BF),
            blocks(16), blocks(16), pltpu.VMEM((D, 16 * TOK), BF), pltpu.VMEM((D, 16 * TOK), BF),
            pltpu.VMEM((16, PAIRS, TOK, TOK), BF), pltpu.VMEM((16, TOK, 2 * TOK), BF), pltpu.VMEM((16, 2 * TOK, D), BF),
            pltpu.VMEM((2, PAIRS, TOK, TOK), BF), pltpu.VMEM((2, 2 * TOK, D), BF),
            blocks(8), pltpu.VMEM((3, units, D), BF), pltpu.VMEM((8 * TOK, D), BF), pltpu.VMEM((3, units, 8 * TOK), BF),
            pltpu.VMEM((TOK, D), F32), pltpu.VMEM((16, 8, D), BF), pltpu.VMEM((15, 8, D), BF), pltpu.VMEM((8, D), BF),
            pltpu.VMEM((16, 8, D), BF), blocks(16), blocks(7), pltpu.VMEM((16, TOK, 2 * TOK), BF),
            sem((6,)), sem((16,)), sem((16,)), sem((17,)), sem((17,)), sem((3,)), sem((3,)), sem((15,)), sem((15,)),
            sem((15,)), sem((15,)), sem((17,)), sem((17,)), sem((15,)), sem((15,)), sem((7,)), sem((7,)),
            sem((3,)), sem((3,)), sem((3,)), sem((32,)),
        ],
        compiler_params=pltpu.CompilerParams(collective_id=0, has_side_effects=True, vmem_limit_bytes=60 * 1024 * 2**10),
        name="split_step",
    )(valid, x, cot, gain, sgain, wq, wkv, wo, wg, wu, wd)


def on_device(
    client_input, client_gain, w_query, w_keyval, w_out, server_gain, w_gate, w_up, w_down, out_grad, valid
):
    parts = step_call(
        valid, client_input[0, 0], out_grad[0, 0], client_gain, server_gain, w_query[0], w_keyval[0], w_out[0],
        w_gate[0].T, w_up[0].T, w_down[0],
    )
    server_out, grad_q, grad_kv, grad_o, gate, up, down = finish_call(*parts)
    return (
        server_out[None, None],
        grad_q[None],
        grad_kv[None],
        grad_o[None],
        gate.T[None],
        up.T[None],
        down[None],
    )


def solution(mesh):
    in_specs = (
        P("grp", "mem", None, None),
        P("mem", None),
        P("mem", None, None),
        P("mem", None, None),
        P("mem", None, None),
        P("grp", None),
        P("grp", None, "mem"),
        P("grp", None, "mem"),
        P("grp", "mem", None),
        P("grp", "mem", None, None),
        P("grp", "mem"),
    )
    out_specs = (
        P("grp", "mem", None, None),
        P("mem", None, None),
        P("mem", None, None),
        P("mem", None, None),
        P("grp", None, "mem"),
        P("grp", None, "mem"),
        P("grp", "mem", None),
    )
    return jax.shard_map(
        on_device, mesh=mesh, in_specs=in_specs, out_specs=out_specs, check_vma=False
    )
```
